16 devices in a mesh: replica: 2 (over y, z), ep: 8 (over x, core).
Axes of the slice: x: 4, y: 2, z: 1, core: 2. Of those that a mesh axis runs over, the one named last changes fastest.
The devices are a block of a 4x4x8 slice.
Arguments:
- tok_in: bfloat16 [8192, 2048], P(('replica', 'ep')), parts along dimension 0
- routes: int32 [2, 8192, 8], P(None, ('replica', 'ep')), parts along dimension 1
- gate_vals: float32 [2, 8192, 8], P(None, ('replica', 'ep')), parts along dimension 1
- w_gate: bfloat16 [2, 32, 2048, 768], P(None, ('replica', 'ep')), parts along dimension 1
- w_up: bfloat16 [2, 32, 2048, 768], P(None, ('replica', 'ep')), parts along dimension 1
- w_down: bfloat16 [2, 32, 768, 2048], P(None, ('replica', 'ep')), parts along dimension 1
- sh_gate: bfloat16 [2, 2048, 768], replicated
- sh_up: bfloat16 [2, 2048, 768], replicated
- sh_down: bfloat16 [2, 768, 2048], replicated
- old_map: int32 [2, 32], P(None, 'replica'), parts along dimension 1
- move_slot: int32 [2, 4], P(None, 'replica'), parts along dimension 1
- move_expert: int32 [2, 4], P(None, 'replica'), parts along dimension 1
Outputs:
- output 1: bfloat16 [8192, 2048], P(('replica', 'ep')), parts along dimension 0
- output 2: bfloat16 [2, 32, 2048, 768], P(None, ('replica', 'ep')), parts along dimension 1
- output 3: bfloat16 [2, 32, 2048, 768], P(None, ('replica', 'ep')), parts along dimension 1
- output 4: bfloat16 [2, 32, 768, 2048], P(None, ('replica', 'ep')), parts along dimension 1
There are 2 independent parts. The reference program is written for one: setup_inputs(seed, part) draws one part's arguments, and reference() takes and returns one part's arrays. A program takes and returns all parts, laid end to end along the dimension named above; an argument that names none is the same for every part.
All inputs are finite; a program needn't handle non-finite values.
Results may differ from the reference program's by a relative error of at most 0.0115771.
Values are sent between devices in bfloat16 or wider.
A program may use at most 768 MiB of HBM per device.

```python
import jax
import jax.numpy as jnp
from jax import lax

HIDDEN = 2048
EXPERT_FF = 768
SHARED_FF = 768
TOP_K = 8
GROUP_DEVS = 8
SLOTS_DEV = 2
TOKENS_DEV = 512
MOVE_COUNT = 2
EXPERTS = 12

SLOT_COUNT = GROUP_DEVS * SLOTS_DEV
TOKEN_COUNT = GROUP_DEVS * TOKENS_DEV
SCORE_RANGE = 2 ** 10
HOT_BONUS = 2 ** 9
COVER_BONUS = 2 ** 12


def draw_layout(rng_key):
    perm_key, extra_key, place_key = jax.random.split(rng_key, 3)
    expert_perm = jax.random.permutation(perm_key, EXPERTS).astype(jnp.int32)
    extra_slot = jax.random.randint(extra_key, (SLOT_COUNT - EXPERTS,), 0, EXPERTS, dtype=jnp.int32)
    canon_old = jnp.concatenate([expert_perm, extra_slot])
    cycled = jnp.concatenate([expert_perm[1:MOVE_COUNT], expert_perm[:1]])
    slot_perm = jax.random.permutation(place_key, SLOT_COUNT).astype(jnp.int32)
    old_map = canon_old[slot_perm]
    slot_of_canon = jnp.argsort(slot_perm).astype(jnp.int32)
    return old_map, slot_of_canon[:MOVE_COUNT], cycled, expert_perm[:MOVE_COUNT]


def draw_routes(rng_key, hot_ids):
    score_key, offset_key = jax.random.split(rng_key)
    score_int = jax.random.randint(score_key, (TOKEN_COUNT, EXPERTS), 0, SCORE_RANGE, dtype=jnp.int32)
    expert_ids = jnp.arange(EXPERTS, dtype=jnp.int32)
    is_hot = jnp.any(expert_ids[:, None] == hot_ids[None, :], axis=1).astype(jnp.int32)
    offset = jax.random.randint(offset_key, (), 0, EXPERTS, dtype=jnp.int32)
    token_ids = jnp.arange(TOKEN_COUNT, dtype=jnp.int32)
    cover_mask = ((token_ids[:, None] + offset) % EXPERTS == expert_ids[None, :]).astype(jnp.int32)
    total_score = score_int + HOT_BONUS * is_hot[None, :] + COVER_BONUS * cover_mask
    picked = lax.top_k(total_score * EXPERTS + expert_ids[None, :], TOP_K)[1]
    return picked.astype(jnp.int32)


def place_slots(expert_w, slot_map):
    return jnp.take(expert_w, slot_map, axis=0)


def setup_inputs(seed: int = 0, part: int = 0) -> dict:
    base_key = jax.random.key(seed)
    part_key = jax.random.fold_in(base_key, part)
    draw_keys = jax.random.split(part_key, 7)
    shared_keys = jax.random.split(jax.random.key(seed + 1), 3)
    old_map, move_slot, move_expert, hot_ids = jax.vmap(draw_layout)(jax.random.split(draw_keys[0], 2))
    routes = jax.vmap(draw_routes)(jax.random.split(draw_keys[1], 2), hot_ids)
    gate_vals = (0.5 + jax.random.uniform(draw_keys[2], (2, TOKEN_COUNT, TOP_K))) / TOP_K ** 0.5
    tok_in = jax.random.normal(draw_keys[3], (TOKEN_COUNT, HIDDEN)).astype(jnp.bfloat16)
    gate_e = (jax.random.normal(draw_keys[4], (2, EXPERTS, HIDDEN, EXPERT_FF)) * HIDDEN ** -0.5).astype(jnp.bfloat16)
    up_e = (jax.random.normal(draw_keys[5], (2, EXPERTS, HIDDEN, EXPERT_FF)) * HIDDEN ** -0.5).astype(jnp.bfloat16)
    down_e = (jax.random.normal(draw_keys[6], (2, EXPERTS, EXPERT_FF, HIDDEN)) * EXPERT_FF ** -0.5).astype(jnp.bfloat16)
    sh_gate = (jax.random.normal(shared_keys[0], (2, HIDDEN, SHARED_FF)) * HIDDEN ** -0.5).astype(jnp.bfloat16)
    sh_up = (jax.random.normal(shared_keys[1], (2, HIDDEN, SHARED_FF)) * HIDDEN ** -0.5).astype(jnp.bfloat16)
    sh_down = (jax.random.normal(shared_keys[2], (2, SHARED_FF, HIDDEN)) * SHARED_FF ** -0.5).astype(jnp.bfloat16)
    return {
        'tok_in': tok_in,
        'routes': routes,
        'gate_vals': gate_vals,
        'w_gate': jax.vmap(place_slots)(gate_e, old_map),
        'w_up': jax.vmap(place_slots)(up_e, old_map),
        'w_down': jax.vmap(place_slots)(down_e, old_map),
        'sh_gate': sh_gate,
        'sh_up': sh_up,
        'sh_down': sh_down,
        'old_map': old_map,
        'move_slot': move_slot,
        'move_expert': move_expert,
    }


def first_holder(slot_map, wanted):
    slot_ids = jnp.arange(SLOT_COUNT, dtype=jnp.int32)
    hit_mask = slot_map[None, :] == wanted[:, None]
    return jnp.min(jnp.where(hit_mask, slot_ids[None, :], SLOT_COUNT), axis=1)


def swiglu(hidden, w_gate, w_up, w_down):
    gate_proj = jnp.dot(hidden, w_gate, preferred_element_type=jnp.float32)
    up_proj = jnp.dot(hidden, w_up, preferred_element_type=jnp.float32)
    inner_act = (jax.nn.silu(gate_proj) * up_proj).astype(jnp.bfloat16)
    return jnp.dot(inner_act, w_down, preferred_element_type=jnp.float32)


def moe_layer(hidden, route_ids, gate_w, w_gate, w_up, w_down, sh_gate, sh_up, sh_down, slot_map):
    expert_ids = jnp.arange(EXPERTS, dtype=jnp.int32)
    holders = first_holder(slot_map, expert_ids)

    def add_expert(running, expert_idx):
        holder_slot = holders[expert_idx]
        expert_out = swiglu(hidden, w_gate[holder_slot], w_up[holder_slot], w_down[holder_slot])
        gate_col = jnp.sum(jnp.where(route_ids == expert_idx, gate_w, 0.0), axis=1)
        return running + gate_col[:, None] * expert_out, None

    start_acc = hidden.astype(jnp.float32) + swiglu(hidden, sh_gate, sh_up, sh_down)
    total_out = lax.scan(add_expert, start_acc, expert_ids)[0]
    return total_out.astype(jnp.bfloat16)


def reference(tok_in, routes, gate_vals, w_gate, w_up, w_down, sh_gate, sh_up, sh_down, old_map, move_slot, move_expert):
    hidden = tok_in
    new_sets = []
    for layer_idx in range(2):
        hidden = moe_layer(hidden, routes[layer_idx], gate_vals[layer_idx], w_gate[layer_idx], w_up[layer_idx], w_down[layer_idx], sh_gate[layer_idx], sh_up[layer_idx], sh_down[layer_idx], old_map[layer_idx])
        new_map = old_map[layer_idx].at[move_slot[layer_idx]].set(move_expert[layer_idx])
        source = first_holder(old_map[layer_idx], new_map)
        new_sets.append((jnp.take(w_gate[layer_idx], source, axis=0), jnp.take(w_up[layer_idx], source, axis=0), jnp.take(w_down[layer_idx], source, axis=0)))
    new_gate = jnp.stack([new_sets[0][0], new_sets[1][0]])
    new_up = jnp.stack([new_sets[0][1], new_sets[1][1]])
    new_down = jnp.stack([new_sets[0][2], new_sets[1][2]])
    return (hidden, new_gate, new_up, new_down)
```

```python
import functools

import jax
import jax.numpy as jnp
from jax import lax
from jax.experimental import pallas as pl
from jax.experimental.pallas import tpu as pltpu
from jax.sharding import PartitionSpec as P

TOKEN_AXES = ('replica', 'ep')
MESH = pl.DeviceIdType.MESH
F32, BF16 = jnp.float32, jnp.bfloat16
CORES = 2
CHUNKS = 8
HALF = CHUNKS // 2
STEPS = 17
LANES = 128
TILE = 256
TILES = 18
LAG = 2
TICKS = TILES + 2 * LAG
RING = 6
PRE = {9: 2, 10: 2, 11: 2, 12: 2, 13: 3, 14: 3, 15: 4, 16: 4}


def moe_kernel(group, inject_ref, coef_ref, tok_ref, wg_ref, wu_ref, wd_ref, sg_ref, su_ref, sd_ref,
               out_ref, pg_ref, pu_ref, pd_ref, arr_ref, far_ref,
               blk, part, rdir, rmrg, xin, wgb, wub, wdb, act, cbuf, ct, colb, pick, land, stage,
               ag_send, ag_recv, fw_send, fw_recv, co_send, co_recv, pw_send, pw_recv,
               di_send, di_recv, xi_send, xi_recv, mg_send, mg_recv, wg_sem, wu_sem, wd_sem, io_sem, out_sem,
               pick_sem, mv_send, mv_recv, arr_sem, far_send, far_recv):
    me = lax.axis_index('ep')
    core = lax.rem(me, CORES)
    chip = me // CORES
    right = lax.rem(me + CORES, group)
    left = lax.rem(me + group - CORES, group)
    mate = me + 1 - 2 * core
    rows_all, width = tok_ref.shape
    ffn = sg_ref.shape[2]
    layers = wg_ref.shape[0]
    slots = wg_ref.shape[1]
    piece = rows_all // CHUNKS
    half_rows = rows_all // 2
    total = layers * STEPS

    def remote(src, dst, send, recv, dev):
        return pltpu.make_async_remote_copy(src_ref=src, dst_ref=dst, send_sem=send, recv_sem=recv,
                                            device_id={'ep': dev}, device_id_type=MESH)

    def rows(c):
        return pl.ds(pl.multiple_of(c * piece, piece), piece)

    def own_copy(side, c):
        late = c // HALF
        return remote(blk.at[0, rows(c)], blk.at[1 + late if side == 0 else 2 - late, rows(c)],
                      ag_send.at[side, c], ag_recv.at[side, c], right if side == 0 else left)

    def forward_copy(side, c):
        at = rows(c + side * HALF)
        return remote(blk.at[1, at], blk.at[3, at], fw_send.at[side, c], fw_recv.at[side, c],
                      right if side == 0 else left)

    def coef_copy(n):
        src, dst, dev = ((0, 1, right), (0, 2, left), (1, 3, right))[n]
        return remote(cbuf.at[src], cbuf.at[dst], co_send.at[n], co_recv.at[n], dev)

    def direct_copy(side, c):
        return remote(part.at[1, rows(c + side * HALF)], rdir.at[side, rows(c)], di_send.at[side, c],
                      di_recv.at[side, c], left if side == 0 else right)

    def relay_copy(side, c):
        return remote(part.at[3, rows(c + side * HALF)], xin.at[side, rows(c)], xi_send.at[side, c],
                      xi_recv.at[side, c], right if side == 0 else left)

    def merged_copy(side, c):
        return remote(part.at[2, rows(c + side * HALF)], rmrg.at[side, rows(c)], mg_send.at[side, c],
                      mg_recv.at[side, c], right if side == 0 else left)

    def mate_copies(l, j):
        return [remote(src.at[l, j], dst.at[l, j], pw_send.at[l, j, n], pw_recv.at[l, j, n], mate)
                for n, (src, dst) in enumerate(((wg_ref, pg_ref), (wu_ref, pu_ref), (wd_ref, pd_ref)))]

    def step_kind(i):
        late = i - 5
        turn = late // 4
        unit = jnp.where(i < 5, 0, jnp.where(turn == 0, 1, 4 - turn))
        pos = jnp.where(i < 5, jnp.where(i < 2, i, jnp.where(i == 2, 4, i - 1)), late - 4 * turn)
        kind = jnp.where(pos == 4, 2, jnp.where(pos < 2, 0, 1))
        return unit, kind, jnp.where(pos == 4, 0, lax.rem(pos, 2))

    def fetch(n, which):
        l = n // STEPS
        i = n - l * STEPS
        _, kind, slot = step_kind(i)
        buf = lax.rem(n, 2)

        def go(g, u, d):
            if which == 0:
                pltpu.make_async_copy(g, wgb.at[buf], wg_sem.at[buf]).start()
                pltpu.make_async_copy(u, wub.at[buf], wu_sem.at[buf]).start()
            else:
                pltpu.make_async_copy(d, wdb, wd_sem).start()

        @pl.when(kind == 0)
        def _():
            go(wg_ref.at[l, slot], wu_ref.at[l, slot], wd_ref.at[l, slot])

        @pl.when(kind == 1)
        def _():
            go(pg_ref.at[l, slot], pu_ref.at[l, slot], pd_ref.at[l, slot])

        @pl.when(kind == 2)
        def _():
            go(sg_ref.at[l], su_ref.at[l], sd_ref.at[l])

    def columns(u, first, second):
        mine = jnp.concatenate([cbuf[first, chip][:, :half_rows], cbuf[second, chip][:, half_rows:]], axis=1)
        full = jnp.concatenate([mine, jnp.zeros((LANES - mine.shape[0], rows_all), F32)], axis=0)
        ct[u] = full.T

    def picks(l, t, side):
        quarter = 2 * core + side
        at = lax.rem(t, 6)

        def pair(own, other, r, c):
            spot = (pl.ds(pl.multiple_of(r, TILE), TILE), pl.ds(pl.multiple_of(c, TILE), TILE))
            return (pltpu.make_async_copy(own.at[(l, slice(None)) + spot], pick.at[side, pl.ds(0, slots)], pick_sem.at[side, 0]),
                    pltpu.make_async_copy(other.at[(l, slice(None)) + spot], pick.at[side, pl.ds(slots, slots)], pick_sem.at[side, 1]))

        tall = 2 * TILE * quarter
        r3, c3 = at // 3, lax.rem(at, 3)
        r2, c2 = at // 2, lax.rem(at, 2)
        return (pair(wg_ref, pg_ref, tall + TILE * r3, TILE * c3), pair(wu_ref, pu_ref, tall + TILE * r3, TILE * c3),
                pair(wd_ref, pd_ref, TILE * r2, tall + TILE * c2))

    def pick_start(l, t):
        for side in range(2):
            for n, pair in enumerate(picks(l, t, side)):
                @pl.when(t // 6 == n)
                def _():
                    for copy in pair:
                        copy.start()

    def tile_copy(tick, side):
        return remote(stage.at[lax.rem(tick, 2), side], land.at[side, lax.rem(tick, RING)], mv_send.at[lax.rem(tick, 2), side],
                      mv_recv.at[side, lax.rem(tick, RING)], right if side == 0 else left)

    def tile_store(l, tick, side):
        return pltpu.make_async_copy(land.at[side, lax.rem(tick, RING)], arr_ref.at[l, side, tick], arr_sem.at[side, lax.rem(tick, 2)])

    def ring_step(l, tick):
        inject = inject_ref[l]
        from_here = inject >= 0
        place = jnp.maximum(inject, 0)

        @pl.when(tick < TILES)
        def _():
            for side in range(2):
                for copy in picks(l, tick, side)[0]:
                    copy.wait()

        for side in range(2):
            @pl.when(tick >= 2)
            def _():
                tile_copy(tick - 2, side).wait_send()

            @pl.when(tick >= LAG)
            def _():
                tile_copy(tick - LAG, side).wait_recv()
                tile_store(l, tick - LAG, side).start()
                stage[lax.rem(tick, 2), side] = jnp.where(from_here, pick[side, place], land[side, lax.rem(tick + RING - LAG, RING)])

            @pl.when(tick < LAG)
            def _():
                stage[lax.rem(tick, 2), side] = pick[side, place]

        @pl.when(tick + 1 < TILES)
        def _():
            pick_start(l, tick + 1)

        for side in range(2):
            @pl.when(tick > LAG)
            def _():
                tile_store(l, tick - LAG - 1, side).wait()

            tile_copy(tick, side).start()

    def ring_finish(l):
        for side in range(2):
            tile_store(l, jnp.int32(TICKS - LAG - 1), side).wait()
            for tick in range(TICKS - LAG, TICKS):
                tile_copy(jnp.int32(tick), side).wait_recv()
                tile_store(l, jnp.int32(tick), side).start()
            for tick in range(TICKS - LAG, TICKS):
                tile_store(l, jnp.int32(tick), side).wait()
                tile_copy(jnp.int32(tick), side).wait_send()
        far_copy(l).start()

    def far_copy(l):
        return remote(arr_ref.at[l], far_ref.at[l], far_send.at[l], far_recv.at[l], mate)

    barrier = pltpu.get_barrier_semaphore()
    for dev in (left, right, mate):
        pl.semaphore_signal(barrier, inc=1, device_id={'ep': dev}, device_id_type=MESH)
    pl.semaphore_wait(barrier, 3)

    tok_in = pltpu.make_async_copy(tok_ref, blk.at[0], io_sem.at[0])
    coef_in = pltpu.make_async_copy(coef_ref, cbuf.at[0], io_sem.at[1])
    tok_in.start()
    coef_in.start()
    fetch(jnp.int32(0), 0)
    fetch(jnp.int32(0), 1)
    tok_in.wait()
    for c in range(CHUNKS):
        own_copy(0, c).start()
        own_copy(1, (c + HALF) % CHUNKS).start()
    coef_in.wait()
    coef_copy(0).start()
    coef_copy(1).start()
    for l in range(layers):
        for j in range(slots):
            for copy in mate_copies(l, j):
                copy.start()
    columns(0, 0, 0)

    @pl.loop(0, layers)
    def layer(l):
        @pl.loop(0, STEPS)
        def step(i):
            n = l * STEPS + i
            unit, kind, slot = step_kind(i)
            buf = lax.rem(n, 2)

            for j, at in ((0, 2), (1, 3)):
                @pl.when(i == at)
                def _():
                    for copy in mate_copies(l, j):
                        copy.wait_recv()

            @pl.when(i == 4)
            def _():
                for c in range(HALF):
                    own_copy(0, c).wait_recv()
                    forward_copy(0, c).start()
                    own_copy(1, c + HALF).wait_recv()
                    forward_copy(1, c).start()
                pick_start(l, jnp.int32(0))

                @pl.when(l == 0)
                def _():
                    coef_copy(0).wait_recv()
                    coef_copy(2).start()
                    coef_copy(1).wait_recv()
                    columns(1, 1, 2)
                    columns(2, 2, 1)

            @pl.when(i == 9)
            def _():
                for c in range(HALF):
                    for side in range(2):
                        forward_copy(side, c).wait()

                @pl.when(l == 0)
                def _():
                    coef_copy(2).wait_recv()
                    columns(3, 3, 3)

            @pl.when(i == 13)
            def _():
                for c in range(HALF):
                    own_copy(0, c + HALF).wait_recv()
                    own_copy(1, c).wait_recv()

            for c in range(HALF):
                @pl.when(i == 9 + c)
                def _():
                    direct_copy(0, c).start()
                    direct_copy(1, c).start()

                @pl.when(i == 13 + c)
                def _():
                    relay_copy(0, c).start()
                    relay_copy(1, c).start()

            first, last = jnp.int32(0), jnp.int32(0)
            done = 0
            for at, count in sorted(PRE.items()):
                first = jnp.where(i == at, done, first)
                last = jnp.where(i == at, min(done + count, TICKS), last)
                done = min(done + count, TICKS)
            assert done == TICKS

            @pl.loop(first, last)
            def _(tick):
                ring_step(l, tick)

            pltpu.make_async_copy(wg_ref.at[0, 0], wgb.at[buf], wg_sem.at[buf]).wait()
            pltpu.make_async_copy(wu_ref.at[0, 0], wub.at[buf], wu_sem.at[buf]).wait()

            @pl.when(n + 1 < total)
            def _():
                fetch(n + 1, 0)

            place = 4 * l + jnp.where(kind == 0, 2 * core, 2 * (1 - core)) + slot
            lane = lax.broadcasted_iota(jnp.int32, (rows_all, LANES), 1)
            col = jnp.sum(jnp.where(lane == place, ct[unit], 0.0), axis=1, keepdims=True)
            col = jnp.where(kind == 2, 1.0, col)
            colb[...] = jnp.broadcast_to(col, (rows_all, LANES))

            @pl.when(i == 0)
            def _():
                part[0] = blk[0].astype(F32)

            @pl.when((i == 5) | (i == 9) | (i == 13))
            def _():
                part[unit] = jnp.zeros((rows_all, width), F32)

            @pl.loop(0, ffn // 256)
            def _(f):
                cols = pl.ds(pl.multiple_of(f * 256, 256), 256)
                gate = jnp.dot(blk[unit], wgb[buf, :, cols], preferred_element_type=F32)
                up = jnp.dot(blk[unit], wub[buf, :, cols], preferred_element_type=F32)
                act[:, cols] = (gate / (1.0 + jnp.exp(-gate)) * up).astype(BF16)

            pltpu.make_async_copy(wd_ref.at[0, 0], wdb, wd_sem).wait()

            @pl.loop(0, width // 512)
            def _(w):
                cols = pl.ds(pl.multiple_of(w * 512, 512), 512)
                down = jnp.dot(act[...], wdb[:, cols], preferred_element_type=F32)
                scale = jnp.concatenate([colb[...]] * 4, axis=1)
                part[unit, :, cols] = part[unit, :, cols] + scale * down

            @pl.when(n + 1 < total)
            def _():
                fetch(n + 1, 1)

        for c in range(CHUNKS):
            own_copy(0, c).wait_send()
            own_copy(1, c).wait_send()

        @pl.loop(0, HALF)
        def merge(c):
            for side in range(2):
                relay_copy(side, c).wait_recv()
                at = rows(c + side * HALF)
                part[2, at] = part[2, at] + xin[side, rows(c)]
            for side in range(2):
                merged_copy(side, c).start()

        ring_finish(l)

        @pl.loop(0, HALF)
        def finish(c):
            for side in range(2):
                direct_copy(side, c).wait_recv()
                merged_copy(side, c).wait_recv()
                d = c + side * HALF
                blk[0, rows(d)] = (part[0, rows(d)] + rdir[side, rows(c)] + rmrg[side, rows(c)]).astype(BF16)

            for side in range(2):
                d = c + side * HALF

                @pl.when(l + 1 < layers)
                def _():
                    own_copy(side, d).start()

                @pl.when(l + 1 == layers)
                def _():
                    pltpu.make_async_copy(blk.at[0, rows(d)], out_ref.at[rows(d)], out_sem.at[side, c]).start()

            for side in range(2):
                @pl.when(l + 1 < layers)
                def _():
                    own_copy(1 - side, c + side * HALF).start()

        for c in range(HALF):
            for side in range(2):
                direct_copy(side, c).wait_send()
                relay_copy(side, c).wait_send()
                merged_copy(side, c).wait_send()

    for c in range(HALF):
        for side in range(2):
            d = c + side * HALF
            pltpu.make_async_copy(blk.at[0, rows(d)], out_ref.at[rows(d)], out_sem.at[side, c]).wait()
    for n in range(3):
        coef_copy(n).wait_send()
    for l in range(layers):
        far_copy(l).wait()
        for j in range(slots):
            for copy in mate_copies(l, j):
                copy.wait_send()


def run_moe(group, inject, coef, tok, w_gate, w_up, w_down, sh_gate, sh_up, sh_down):
    n_rows, width = tok.shape
    layers, slots, _, ffn = w_gate.shape
    half = n_rows // 2
    chips = group // CORES
    any_spec = pl.BlockSpec(memory_space=pl.ANY)
    dma = pltpu.SemaphoreType.DMA
    flops = 2 * n_rows * 3 * width * ffn * layers * STEPS
    arrivals = jax.ShapeDtypeStruct((layers, 2, TICKS, TILE, TILE), BF16)
    return pl.pallas_call(
        functools.partial(moe_kernel, group),
        name='moe',
        out_shape=(jax.ShapeDtypeStruct(tok.shape, BF16),) + tuple(
            jax.ShapeDtypeStruct(w.shape, BF16) for w in (w_gate, w_up, w_down)) + (arrivals, arrivals),
        in_specs=[pl.BlockSpec(memory_space=pltpu.SMEM)] + [any_spec] * 8,
        out_specs=[any_spec] * 6,
        scratch_shapes=[
            pltpu.VMEM((chips, n_rows, width), BF16),
            pltpu.VMEM((chips, n_rows, width), F32),
            pltpu.VMEM((2, half, width), F32),
            pltpu.VMEM((2, half, width), F32),
            pltpu.VMEM((2, half, width), F32),
            pltpu.VMEM((2, width, ffn), BF16),
            pltpu.VMEM((2, width, ffn), BF16),
            pltpu.VMEM((ffn, width), BF16),
            pltpu.VMEM((n_rows, ffn), BF16),
            pltpu.VMEM((chips,) + coef.shape, F32),
            pltpu.VMEM((chips, n_rows, LANES), F32),
            pltpu.VMEM((n_rows, LANES), F32),
            pltpu.VMEM((2, CORES * slots, TILE, TILE), BF16),
            pltpu.VMEM((2, RING, TILE, TILE), BF16),
            pltpu.VMEM((2, 2, TILE, TILE), BF16),
            dma((2, CHUNKS)), dma((2, CHUNKS)), dma((2, HALF)), dma((2, HALF)), dma((3,)), dma((3,)),
            dma((layers, slots, 3)), dma((layers, slots, 3)),
            dma((2, HALF)), dma((2, HALF)), dma((2, HALF)), dma((2, HALF)), dma((2, HALF)), dma((2, HALF)),
            dma((2,)), dma((2,)), dma, dma((2,)), dma((2, HALF)),
            dma((2, 2)), dma((2, 2)), dma((2, RING)), dma((2, 2)), dma((layers,)), dma((layers,)),
        ],
        compiler_params=pltpu.CompilerParams(collective_id=0, has_side_effects=True, vmem_limit_bytes=67043328),
        cost_estimate=pl.CostEstimate(flops=flops, bytes_accessed=400 * 2 ** 20, transcendentals=0),
    )(inject, coef, tok, w_gate, w_up, w_down, sh_gate, sh_up, sh_down)


KEEP, NEAR, RINGED = 0, 1, 2
DEPTH = 4


def place_kernel(table_ref, core_ref, wg_ref, wu_ref, wd_ref, pg_ref, pu_ref, pd_ref, arr_ref, far_ref,
                 ng_ref, nu_ref, nd_ref, tall, wide, in_sem, out_sem):
    layers, slots = wg_ref.shape[:2]
    core = core_ref[0]
    jobs = [(l, j, n) for l in range(layers) for j in range(slots) for n in range(3)]

    def parts(k):
        l, j, n = jobs[k]
        own = (wg_ref, wu_ref, wd_ref)[n]
        other = (pg_ref, pu_ref, pd_ref)[n]
        new = (ng_ref, nu_ref, nd_ref)[n]
        buf = (wide if n == 2 else tall).at[k % DEPTH]
        return l, j, n, own, other, new, buf

    def load(k):
        l, j, n, own, other, new, buf = parts(k)
        mode, pos = table_ref[l, j, 0], table_ref[l, j, 1]
        sem = in_sem.at[k % DEPTH]

        @pl.when(mode == KEEP)
        def _():
            pltpu.make_async_copy(own.at[l, j], buf, sem).start()

        @pl.when((mode == NEAR) & (pos < slots))
        def _():
            pltpu.make_async_copy(own.at[l, pos], buf, sem).start()

        @pl.when((mode == NEAR) & (pos >= slots))
        def _():
            pltpu.make_async_copy(other.at[l, pos - slots], buf, sem).start()

        @pl.when(mode == RINGED)
        def _():
            for side in range(2):
                start = table_ref[l, j, 2 + side] + 6 * n
                for source, owner in ((arr_ref, core), (far_ref, 1 - core)):
                    tall_at = 2 * TILE * (2 * owner + side)

                    @pl.loop(0, 6)
                    def _(t):
                        if n == 2:
                            r, c = TILE * (t // 2), tall_at + TILE * lax.rem(t, 2)
                        else:
                            r, c = tall_at + TILE * (t // 3), TILE * lax.rem(t, 3)
                        spot = (pl.ds(pl.multiple_of(r, TILE), TILE), pl.ds(pl.multiple_of(c, TILE), TILE))
                        pltpu.make_async_copy(source.at[l, side, start + t], buf.at[spot], sem).start()

    def arrive(k):
        l, j, n, own, other, new, buf = parts(k)
        pltpu.make_async_copy(own.at[l, j], buf, in_sem.at[k % DEPTH]).wait()

    def store(k):
        l, j, n, own, other, new, buf = parts(k)
        return pltpu.make_async_copy(buf, new.at[l, j], out_sem.at[k % DEPTH])

    ahead = DEPTH - 1
    for k in range(ahead):
        load(k)
    for k in range(len(jobs)):
        arrive(k)
        store(k).start()
        if k >= 1:
            store(k - 1).wait()
        if k + ahead < len(jobs):
            load(k + ahead)
    store(len(jobs) - 1).wait()


def run_place(table, core, w_gate, w_up, w_down, p_gate, p_up, p_down, arrived, far):
    _, _, width, ffn = w_gate.shape
    any_spec = pl.BlockSpec(memory_space=pl.ANY)
    smem = pl.BlockSpec(memory_space=pltpu.SMEM)
    dma = pltpu.SemaphoreType.DMA
    return pl.pallas_call(
        place_kernel,
        name='place',
        out_shape=tuple(jax.ShapeDtypeStruct(w.shape, BF16) for w in (w_gate, w_up, w_down)),
        in_specs=[smem, smem] + [any_spec] * 8,
        out_specs=[any_spec] * 3,
        scratch_shapes=[pltpu.VMEM((DEPTH, width, ffn), BF16), pltpu.VMEM((DEPTH, ffn, width), BF16), dma((DEPTH,)), dma((DEPTH,))],
        compiler_params=pltpu.CompilerParams(vmem_limit_bytes=48 * 2 ** 20),
    )(table, core, w_gate, w_up, w_down, p_gate, p_up, p_down, arrived, far)


def coefficients(routes, gate_vals, old_map, chips):
    layers, n_rows, _ = routes.shape
    n_slots = old_map.shape[1]
    ids = jnp.arange(n_slots, dtype=jnp.int32)
    earlier = (old_map[:, :, None] == old_map[:, None, :]) & (ids[None, :] < ids[:, None])[None]
    serve = jnp.where(jnp.any(earlier, axis=2), 0.0, 1.0)
    hit = routes[:, :, :, None] == old_map[:, None, None, :]
    coef = jnp.sum(jnp.where(hit, gate_vals[..., None], 0.0), axis=2) * serve[:, None, :]
    coef = coef.transpose(2, 0, 1).reshape(chips, n_slots // chips, layers, n_rows)
    return coef.transpose(0, 2, 1, 3).reshape(chips, layers * (n_slots // chips), n_rows)


def plan(old_map, move_slot, move_expert, chips, me, slots):
    layers, n_slots = old_map.shape
    per_chip = n_slots // chips
    chip, core = me // CORES, me % CORES
    holds = (old_map[:, None, :] == move_expert[:, :, None]).reshape(layers, 2, chips, per_chip)
    on_chip = jnp.any(holds, axis=3)
    spot = jnp.argmax(holds, axis=3).astype(jnp.int32)
    first = jnp.argmax(on_chip, axis=2).astype(jnp.int32)
    target = move_slot // per_chip

    def has(m, x):
        return jnp.take_along_axis(on_chip[:, m], x[:, None], axis=1)[:, 0]

    b0, b1 = target[:, 0], target[:, 1]
    near0, near1 = has(0, b0), has(1, b1)
    swap = has(0, b1) & has(1, b0)
    neither = ~near0 & ~near1
    a0 = jnp.where(near0, b0, jnp.where(neither & swap, b1, first[:, 0]))
    a1 = jnp.where(near1, b1, jnp.where(neither & swap, b0, first[:, 1]))
    left_over = neither & ~swap

    def position(index):
        return jnp.where(index // slots == core, index % slots, slots + index % slots)

    source = jnp.stack([a0, a1], axis=1)
    active = (source != target) & jnp.stack([jnp.ones_like(left_over), ~left_over], axis=1)
    here = jnp.where(active & (source == chip), position(spot[:, :, chip]), -1)
    inject = jnp.max(here, axis=1)

    mine = me * slots + jnp.arange(slots, dtype=jnp.int32)
    hit = move_slot[:, None, :] == mine[None, :, None]
    near = jnp.stack([near0, near1], axis=1)
    kind = jnp.where(near, NEAR, jnp.where(active, RINGED, KEEP))
    pos = position(spot[:, :, chip])
    ahead = (target - source) % chips
    fields = jnp.stack([kind, pos, (ahead - 1) * LAG, (chips - ahead - 1) * LAG], axis=2)
    table = jnp.sum(jnp.where(hit[..., None], fields[:, None], 0), axis=2)
    return inject.astype(jnp.int32), table.astype(jnp.int32), left_over


def finish_moves(news, weights, left_over, old_map, move_slot, move_expert, me, slots):
    layers, n_slots = old_map.shape
    ids = jnp.arange(n_slots, dtype=jnp.int32)
    source = jnp.min(jnp.where(old_map == move_expert[:, 1:], ids[None, :], n_slots), axis=1)
    order = jnp.argsort(~left_over)

    def one(k, news):
        l = order[k]
        here = source[l] // slots == me
        there = move_slot[l, 1] // slots == me
        index = move_slot[l, 1] % slots
        out = []
        for new, w in zip(news, weights):
            sent = jnp.where(here, w[l, source[l] % slots], jnp.zeros((), w.dtype))
            got = lax.psum(sent, 'ep')
            out.append(new.at[l, index].set(jnp.where(there, got, new[l, index])))
        return tuple(out)

    return lax.fori_loop(0, jnp.sum(left_over.astype(jnp.int32)), one, news)


def solution(mesh):
    group = mesh.shape['ep']

    def body(tok_in, routes, gate_vals, w_gate, w_up, w_down, sh_gate, sh_up, sh_down, old_map, move_slot, move_expert):
        me = lax.axis_index('ep')
        slots = w_gate.shape[1]
        chips = group // CORES
        coef = coefficients(routes, gate_vals, old_map, chips)
        inject, table, left_over = plan(old_map, move_slot, move_expert, chips, me, slots)
        hidden, p_gate, p_up, p_down, arrived, far = run_moe(group, inject, coef, tok_in, w_gate, w_up, w_down, sh_gate, sh_up, sh_down)
        core = (me % CORES).astype(jnp.int32).reshape(1)
        news = run_place(table, core, w_gate, w_up, w_down, p_gate, p_up, p_down, arrived, far)
        news = finish_moves(news, (w_gate, w_up, w_down), left_over, old_map, move_slot, move_expert, me, slots)
        return (hidden,) + tuple(news)

    weight_spec = P(None, TOKEN_AXES, None, None)
    route_spec = P(None, TOKEN_AXES, None)
    map_spec = P(None, 'replica')
    shared_spec = P(None, None, None)
    tok_spec = P(TOKEN_AXES, None)
    return jax.shard_map(body, mesh=mesh, in_specs=(tok_spec, route_spec, route_spec, weight_spec, weight_spec, weight_spec, shared_spec, shared_spec, shared_spec, map_spec, map_spec, map_spec), out_specs=(tok_spec, weight_spec, weight_spec, weight_spec), check_vma=False)
```

```python
import functools

import jax
import jax.numpy as jnp
from jax import lax
from jax.experimental import pallas as pl
from jax.experimental.pallas import tpu as pltpu
from jax.sharding import PartitionSpec as P

TOKEN_AXES = ('replica', 'ep')
MESH = pl.DeviceIdType.MESH
F32, BF16 = jnp.float32, jnp.bfloat16
CORES = 2
CHUNKS = 8
HALF = CHUNKS // 2
STEPS = 17
LANES = 128
TILE = 256
TILES = 18
LAG = 2
TICKS = TILES + 2 * LAG
RING = 6
PRE = {9: 2, 10: 2, 11: 2, 12: 2, 13: 3, 14: 3, 15: 4, 16: 4}


def read_plan(map_ref, slot_ref, expert_ref, l, chips, per_chip, chip, core, slots):
    def place_on(m, x):
        found = per_chip
        for a in reversed(range(per_chip)):
            found = jnp.where(map_ref[l, x * per_chip + a] == expert_ref[l, m], a, found)
        return found

    spots = [[place_on(m, x) for x in range(chips)] for m in range(2)]
    held = [[s < per_chip for s in row] for row in spots]
    goals = []
    for m in range(2):
        to = slot_ref[l, m]
        goal = 0
        for x in range(1, chips):
            goal = jnp.where(to >= x * per_chip, x, goal)
        goals.append(goal)

    def has(m, x):
        out = held[m][0] & (x == 0)
        for c in range(1, chips):
            out = out | (held[m][c] & (x == c))
        return out

    def lowest(m):
        out = chips - 1
        for c in reversed(range(chips - 1)):
            out = jnp.where(held[m][c], c, out)
        return out

    near = [has(m, goals[m]) for m in range(2)]
    neither = jnp.logical_not(near[0] | near[1])
    swap = neither & has(0, goals[1]) & has(1, goals[0])
    left_over = neither & jnp.logical_not(swap)
    origin = [jnp.where(near[m], goals[m], jnp.where(swap, goals[1 - m], lowest(m))) for m in range(2)]
    ringed = [jnp.logical_not(near[0]), jnp.logical_not(near[1] | left_over)]
    places = []
    for m in range(2):
        a = jnp.int32(0)
        for x in range(chips):
            a = jnp.where(chip == x, spots[m][x], a)
        mine = (a >= core * slots) & (a < (core + 1) * slots)
        places.append(jnp.where(mine, a - core * slots, slots + a - (1 - core) * slots))
    return goals, origin, near, ringed, left_over, places


def moe_kernel(group, map_ref, slot_ref, expert_ref, route_ref, gate_ref, tok_ref, wg_ref, wu_ref, wd_ref, sg_ref, su_ref, sd_ref,
               out_ref, pg_ref, pu_ref, pd_ref, arr_ref, far_ref,
               blk, part, rdir, rmrg, xin, wgb, wub, wdb, act, rbuf, gbuf, cbuf, ct, colb, pick, land, stage,
               ag_send, ag_recv, fw_send, fw_recv, co_send, co_recv, pw_send, pw_recv,
               di_send, di_recv, xi_send, xi_recv, mg_send, mg_recv, wg_sem, wu_sem, wd_sem, io_sem, out_sem,
               pick_sem, mv_send, mv_recv, arr_sem, far_send, far_recv):
    me = lax.axis_index('ep')
    core = lax.rem(me, CORES)
    chip = me // CORES
    right = lax.rem(me + CORES, group)
    left = lax.rem(me + group - CORES, group)
    mate = me + 1 - 2 * core
    rows_all, width = tok_ref.shape
    ffn = sg_ref.shape[2]
    layers = wg_ref.shape[0]
    slots = wg_ref.shape[1]
    piece = rows_all // CHUNKS
    half_rows = rows_all // 2
    total = layers * STEPS
    chips = group // CORES
    n_slots = group * slots

    def remote(src, dst, send, recv, dev):
        return pltpu.make_async_remote_copy(src_ref=src, dst_ref=dst, send_sem=send, recv_sem=recv,
                                            device_id={'ep': dev}, device_id_type=MESH)

    def rows(c):
        return pl.ds(pl.multiple_of(c * piece, piece), piece)

    def own_copy(side, c):
        late = c // HALF
        return remote(blk.at[0, rows(c)], blk.at[1 + late if side == 0 else 2 - late, rows(c)],
                      ag_send.at[side, c], ag_recv.at[side, c], right if side == 0 else left)

    def forward_copy(side, c):
        at = rows(c + side * HALF)
        return remote(blk.at[1, at], blk.at[3, at], fw_send.at[side, c], fw_recv.at[side, c],
                      right if side == 0 else left)

    def coef_copy(n):
        src, dst, dev = ((0, 1, right), (0, 2, left), (1, 3, right))[n]
        return remote(cbuf.at[src], cbuf.at[dst], co_send.at[n], co_recv.at[n], dev)

    def direct_copy(side, c):
        return remote(part.at[1, rows(c + side * HALF)], rdir.at[side, rows(c)], di_send.at[side, c],
                      di_recv.at[side, c], left if side == 0 else right)

    def relay_copy(side, c):
        return remote(part.at[3, rows(c + side * HALF)], xin.at[side, rows(c)], xi_send.at[side, c],
                      xi_recv.at[side, c], right if side == 0 else left)

    def merged_copy(side, c):
        return remote(part.at[2, rows(c + side * HALF)], rmrg.at[side, rows(c)], mg_send.at[side, c],
                      mg_recv.at[side, c], right if side == 0 else left)

    def mate_copies(l, j):
        return [remote(src.at[l, j], dst.at[l, j], pw_send.at[l, j, n], pw_recv.at[l, j, n], mate)
                for n, (src, dst) in enumerate(((wg_ref, pg_ref), (wu_ref, pu_ref), (wd_ref, pd_ref)))]

    def step_kind(i):
        late = i - 5
        turn = late // 4
        unit = jnp.where(i < 5, 0, jnp.where(turn == 0, 1, 4 - turn))
        pos = jnp.where(i < 5, jnp.where(i < 2, i, jnp.where(i == 2, 4, i - 1)), late - 4 * turn)
        kind = jnp.where(pos == 4, 2, jnp.where(pos < 2, 0, 1))
        return unit, kind, jnp.where(pos == 4, 0, lax.rem(pos, 2))

    def fetch(n, which):
        l = n // STEPS
        i = n - l * STEPS
        _, kind, slot = step_kind(i)
        buf = lax.rem(n, 2)

        def go(g, u, d):
            if which == 0:
                pltpu.make_async_copy(g, wgb.at[buf], wg_sem.at[buf]).start()
                pltpu.make_async_copy(u, wub.at[buf], wu_sem.at[buf]).start()
            else:
                pltpu.make_async_copy(d, wdb, wd_sem).start()

        @pl.when(kind == 0)
        def _():
            go(wg_ref.at[l, slot], wu_ref.at[l, slot], wd_ref.at[l, slot])

        @pl.when(kind == 1)
        def _():
            go(pg_ref.at[l, slot], pu_ref.at[l, slot], pd_ref.at[l, slot])

        @pl.when(kind == 2)
        def _():
            go(sg_ref.at[l], su_ref.at[l], sd_ref.at[l])

    def columns(u, first, second):
        mine = jnp.concatenate([cbuf[first, chip][:, :half_rows], cbuf[second, chip][:, half_rows:]], axis=1)
        full = jnp.concatenate([mine, jnp.zeros((LANES - mine.shape[0], rows_all), F32)], axis=0)
        ct[u] = full.T

    def picks(l, t, side):
        quarter = 2 * core + side
        at = lax.rem(t, 6)

        def pair(own, other, r, c):
            spot = (pl.ds(pl.multiple_of(r, TILE), TILE), pl.ds(pl.multiple_of(c, TILE), TILE))
            return (pltpu.make_async_copy(own.at[(l, slice(None)) + spot], pick.at[side, pl.ds(0, slots)], pick_sem.at[side, 0]),
                    pltpu.make_async_copy(other.at[(l, slice(None)) + spot], pick.at[side, pl.ds(slots, slots)], pick_sem.at[side, 1]))

        tall = 2 * TILE * quarter
        r3, c3 = at // 3, lax.rem(at, 3)
        r2, c2 = at // 2, lax.rem(at, 2)
        return (pair(wg_ref, pg_ref, tall + TILE * r3, TILE * c3), pair(wu_ref, pu_ref, tall + TILE * r3, TILE * c3),
                pair(wd_ref, pd_ref, TILE * r2, tall + TILE * c2))

    def pick_start(l, t):
        for side in range(2):
            for n, pair in enumerate(picks(l, t, side)):
                @pl.when(t // 6 == n)
                def _():
                    for copy in pair:
                        copy.start()

    def tile_copy(tick, side):
        return remote(stage.at[lax.rem(tick, 2), side], land.at[side, lax.rem(tick, RING)], mv_send.at[lax.rem(tick, 2), side],
                      mv_recv.at[side, lax.rem(tick, RING)], right if side == 0 else left)

    def tile_store(l, tick, side):
        return pltpu.make_async_copy(land.at[side, lax.rem(tick, RING)], arr_ref.at[l, side, tick], arr_sem.at[side, lax.rem(tick, 2)])

    def ring_step(l, tick):
        _, origin, _, ringed, _, places = read_plan(map_ref, slot_ref, expert_ref, l, chips, CORES * slots, chip, core, slots)
        sends = [ringed[m] & (origin[m] == chip) for m in range(2)]
        from_here = sends[0] | sends[1]
        place = jnp.where(sends[0], places[0], jnp.where(sends[1], places[1], 0))

        @pl.when(tick < TILES)
        def _():
            for side in range(2):
                for copy in picks(l, tick, side)[0]:
                    copy.wait()

        for side in range(2):
            @pl.when(tick >= 2)
            def _():
                tile_copy(tick - 2, side).wait_send()

            @pl.when(tick >= LAG)
            def _():
                tile_copy(tick - LAG, side).wait_recv()
                tile_store(l, tick - LAG, side).start()
                stage[lax.rem(tick, 2), side] = jnp.where(from_here, pick[side, place], land[side, lax.rem(tick + RING - LAG, RING)])

            @pl.when(tick < LAG)
            def _():
                stage[lax.rem(tick, 2), side] = pick[side, place]

        @pl.when(tick + 1 < TILES)
        def _():
            pick_start(l, tick + 1)

        for side in range(2):
            @pl.when(tick > LAG)
            def _():
                tile_store(l, tick - LAG - 1, side).wait()

            tile_copy(tick, side).start()

    def ring_finish(l):
        for side in range(2):
            tile_store(l, jnp.int32(TICKS - LAG - 1), side).wait()
            for tick in range(TICKS - LAG, TICKS):
                tile_copy(jnp.int32(tick), side).wait_recv()
                tile_store(l, jnp.int32(tick), side).start()
            for tick in range(TICKS - LAG, TICKS):
                tile_store(l, jnp.int32(tick), side).wait()
                tile_copy(jnp.int32(tick), side).wait_send()
        far_copy(l).start()

    def far_copy(l):
        return remote(arr_ref.at[l], far_ref.at[l], far_send.at[l], far_recv.at[l], mate)

    tok_in = pltpu.make_async_copy(tok_ref, blk.at[0], io_sem.at[0])
    route_in = pltpu.make_async_copy(route_ref, rbuf, io_sem.at[1])
    gate_in = pltpu.make_async_copy(gate_ref, gbuf, io_sem.at[2])
    tok_in.start()
    route_in.start()
    gate_in.start()
    fetch(jnp.int32(0), 0)
    fetch(jnp.int32(0), 1)

    barrier = pltpu.get_barrier_semaphore()
    for dev in (left, right, mate):
        pl.semaphore_signal(barrier, inc=1, device_id={'ep': dev}, device_id_type=MESH)
    pl.semaphore_wait(barrier, 3)

    tok_in.wait()
    for c in range(CHUNKS):
        own_copy(0, c).start()
        own_copy(1, (c + HALF) % CHUNKS).start()
    for l in range(layers):
        for j in range(slots):
            for copy in mate_copies(l, j):
                copy.start()

    route_in.wait()
    gate_in.wait()
    for l in range(layers):
        for q in range(n_slots):
            expert = map_ref[l, q]
            serves = jnp.float32(1.0)
            for p in range(q):
                serves = jnp.where(map_ref[l, p] == expert, 0.0, serves)
            gates = jnp.sum(jnp.where(rbuf[l] == expert, gbuf[l], 0.0), axis=0, keepdims=True)
            at = slots * CORES * l + q % (slots * CORES)
            cbuf[0, q // (slots * CORES), at:at + 1, :] = gates * serves
    coef_copy(0).start()
    coef_copy(1).start()
    columns(0, 0, 0)

    @pl.loop(0, layers)
    def layer(l):
        @pl.loop(0, STEPS)
        def step(i):
            n = l * STEPS + i
            unit, kind, slot = step_kind(i)
            buf = lax.rem(n, 2)

            for j, at in ((0, 2), (1, 3)):
                @pl.when(i == at)
                def _():
                    for copy in mate_copies(l, j):
                        copy.wait_recv()

            @pl.when(i == 4)
            def _():
                for c in range(HALF):
                    own_copy(0, c).wait_recv()
                    forward_copy(0, c).start()
                    own_copy(1, c + HALF).wait_recv()
                    forward_copy(1, c).start()
                pick_start(l, jnp.int32(0))

                @pl.when(l == 0)
                def _():
                    coef_copy(0).wait_recv()
                    coef_copy(2).start()
                    coef_copy(1).wait_recv()
                    columns(1, 1, 2)
                    columns(2, 2, 1)

            @pl.when(i == 9)
            def _():
                for c in range(HALF):
                    for side in range(2):
                        forward_copy(side, c).wait()

                @pl.when(l == 0)
                def _():
                    coef_copy(2).wait_recv()
                    columns(3, 3, 3)

            @pl.when(i == 13)
            def _():
                for c in range(HALF):
                    own_copy(0, c + HALF).wait_recv()
                    own_copy(1, c).wait_recv()

            for c in range(HALF):
                @pl.when(i == 9 + c)
                def _():
                    direct_copy(0, c).start()
                    direct_copy(1, c).start()

                @pl.when(i == 13 + c)
                def _():
                    relay_copy(0, c).start()
                    relay_copy(1, c).start()

            first, last = jnp.int32(0), jnp.int32(0)
            done = 0
            for at, count in sorted(PRE.items()):
                first = jnp.where(i == at, done, first)
                last = jnp.where(i == at, min(done + count, TICKS), last)
                done = min(done + count, TICKS)
            assert done == TICKS

            @pl.loop(first, last)
            def _(tick):
                ring_step(l, tick)

            pltpu.make_async_copy(wg_ref.at[0, 0], wgb.at[buf], wg_sem.at[buf]).wait()
            pltpu.make_async_copy(wu_ref.at[0, 0], wub.at[buf], wu_sem.at[buf]).wait()

            @pl.when(n + 1 < total)
            def _():
                fetch(n + 1, 0)

            place = 4 * l + jnp.where(kind == 0, 2 * core, 2 * (1 - core)) + slot
            lane = lax.broadcasted_iota(jnp.int32, (rows_all, LANES), 1)
            col = jnp.sum(jnp.where(lane == place, ct[unit], 0.0), axis=1, keepdims=True)
            col = jnp.where(kind == 2, 1.0, col)
            colb[...] = jnp.broadcast_to(col, (rows_all, LANES))

            @pl.when(i == 0)
            def _():
                part[0] = blk[0].astype(F32)

            @pl.when((i == 5) | (i == 9) | (i == 13))
            def _():
                part[unit] = jnp.zeros((rows_all, width), F32)

            @pl.loop(0, ffn // 256)
            def _(f):
                cols = pl.ds(pl.multiple_of(f * 256, 256), 256)
                gate = jnp.dot(blk[unit], wgb[buf, :, cols], preferred_element_type=F32)
                up = jnp.dot(blk[unit], wub[buf, :, cols], preferred_element_type=F32)
                act[:, cols] = (gate / (1.0 + jnp.exp(-gate)) * up).astype(BF16)

            pltpu.make_async_copy(wd_ref.at[0, 0], wdb, wd_sem).wait()

            @pl.loop(0, width // 512)
            def _(w):
                cols = pl.ds(pl.multiple_of(w * 512, 512), 512)
                down = jnp.dot(act[...], wdb[:, cols], preferred_element_type=F32)
                scale = jnp.concatenate([colb[...]] * 4, axis=1)
                part[unit, :, cols] = part[unit, :, cols] + scale * down

            @pl.when(n + 1 < total)
            def _():
                fetch(n + 1, 1)

        for c in range(CHUNKS):
            own_copy(0, c).wait_send()
            own_copy(1, c).wait_send()

        @pl.loop(0, HALF)
        def merge(c):
            for side in range(2):
                relay_copy(side, c).wait_recv()
                at = rows(c + side * HALF)
                part[2, at] = part[2, at] + xin[side, rows(c)]
            for side in range(2):
                merged_copy(side, c).start()

        ring_finish(l)

        @pl.loop(0, HALF)
        def finish(c):
            for side in range(2):
                direct_copy(side, c).wait_recv()
                merged_copy(side, c).wait_recv()
                d = c + side * HALF
                blk[0, rows(d)] = (part[0, rows(d)] + rdir[side, rows(c)] + rmrg[side, rows(c)]).astype(BF16)

            for side in range(2):
                d = c + side * HALF

                @pl.when(l + 1 < layers)
                def _():
                    own_copy(side, d).start()

                @pl.when(l + 1 == layers)
                def _():
                    pltpu.make_async_copy(blk.at[0, rows(d)], out_ref.at[rows(d)], out_sem.at[side, c]).start()

            for side in range(2):
                @pl.when(l + 1 < layers)
                def _():
                    own_copy(1 - side, c + side * HALF).start()

        for c in range(HALF):
            for side in range(2):
                direct_copy(side, c).wait_send()
                relay_copy(side, c).wait_send()
                merged_copy(side, c).wait_send()

    for c in range(HALF):
        for side in range(2):
            d = c + side * HALF
            pltpu.make_async_copy(blk.at[0, rows(d)], out_ref.at[rows(d)], out_sem.at[side, c]).wait()
    for n in range(3):
        coef_copy(n).wait_send()
    for l in range(layers):
        far_copy(l).wait()
        for j in range(slots):
            for copy in mate_copies(l, j):
                copy.wait_send()


def run_moe(group, old_map, move_slot, move_expert, routes, gates, tok, w_gate, w_up, w_down, sh_gate, sh_up, sh_down):
    n_rows, width = tok.shape
    layers, slots, _, ffn = w_gate.shape
    half = n_rows // 2
    chips = group // CORES
    any_spec = pl.BlockSpec(memory_space=pl.ANY)
    dma = pltpu.SemaphoreType.DMA
    flops = 2 * n_rows * 3 * width * ffn * layers * STEPS
    arrivals = jax.ShapeDtypeStruct((layers, 2, TICKS, TILE, TILE), BF16)
    return pl.pallas_call(
        functools.partial(moe_kernel, group),
        name='moe',
        out_shape=(jax.ShapeDtypeStruct(tok.shape, BF16),) + tuple(
            jax.ShapeDtypeStruct(w.shape, BF16) for w in (w_gate, w_up, w_down)) + (arrivals, arrivals),
        in_specs=[pl.BlockSpec(memory_space=pltpu.SMEM)] * 3 + [any_spec] * 9,
        out_specs=[any_spec] * 6,
        scratch_shapes=[
            pltpu.VMEM((chips, n_rows, width), BF16),
            pltpu.VMEM((chips, n_rows, width), F32),
            pltpu.VMEM((2, half, width), F32),
            pltpu.VMEM((2, half, width), F32),
            pltpu.VMEM((2, half, width), F32),
            pltpu.VMEM((2, width, ffn), BF16),
            pltpu.VMEM((2, width, ffn), BF16),
            pltpu.VMEM((ffn, width), BF16),
            pltpu.VMEM((n_rows, ffn), BF16),
            pltpu.VMEM(routes.shape, jnp.int32),
            pltpu.VMEM(gates.shape, F32),
            pltpu.VMEM((chips, chips, layers * slots * CORES, n_rows), F32),
            pltpu.VMEM((chips, n_rows, LANES), F32),
            pltpu.VMEM((n_rows, LANES), F32),
            pltpu.VMEM((2, CORES * slots, TILE, TILE), BF16),
            pltpu.VMEM((2, RING, TILE, TILE), BF16),
            pltpu.VMEM((2, 2, TILE, TILE), BF16),
            dma((2, CHUNKS)), dma((2, CHUNKS)), dma((2, HALF)), dma((2, HALF)), dma((3,)), dma((3,)),
            dma((layers, slots, 3)), dma((layers, slots, 3)),
            dma((2, HALF)), dma((2, HALF)), dma((2, HALF)), dma((2, HALF)), dma((2, HALF)), dma((2, HALF)),
            dma((2,)), dma((2,)), dma, dma((3,)), dma((2, HALF)),
            dma((2, 2)), dma((2, 2)), dma((2, RING)), dma((2, 2)), dma((layers,)), dma((layers,)),
        ],
        compiler_params=pltpu.CompilerParams(collective_id=0, has_side_effects=True, vmem_limit_bytes=67043328),
        cost_estimate=pl.CostEstimate(flops=flops, bytes_accessed=400 * 2 ** 20, transcendentals=0),
    )(old_map, move_slot, move_expert, routes, gates, tok, w_gate, w_up, w_down, sh_gate, sh_up, sh_down)


KEEP, NEAR, RINGED = 0, 1, 2
DEPTH = 4


def place_kernel(group, map_ref, slot_ref, expert_ref, wg_ref, wu_ref, wd_ref, pg_ref, pu_ref, pd_ref, arr_ref, far_ref,
                 ng_ref, nu_ref, nd_ref, over_ref, tall, wide, in_sem, out_sem):
    layers, slots = wg_ref.shape[:2]
    me = lax.axis_index('ep')
    core = lax.rem(me, CORES)
    chip = me // CORES
    chips = group // CORES
    table = {}
    for l in range(layers):
        goals, origin, near, ringed, left_over, places = read_plan(map_ref, slot_ref, expert_ref, l, chips, CORES * slots, chip, core, slots)
        over_ref[l] = left_over.astype(jnp.int32)
        for j in range(slots):
            mode, pos, first, second = KEEP, 0, 0, 0
            for m in range(2):
                here = slot_ref[l, m] == me * slots + j
                ahead = lax.rem(goals[m] - origin[m] + chips, chips)
                mode = jnp.where(here, jnp.where(near[m], NEAR, jnp.where(ringed[m], RINGED, KEEP)), mode)
                pos = jnp.where(here, places[m], pos)
                first = jnp.where(here, (ahead - 1) * LAG, first)
                second = jnp.where(here, (chips - ahead - 1) * LAG, second)
            table[l, j] = mode, pos, (first, second)
    jobs = [(l, j, n) for l in range(layers) for j in range(slots) for n in range(3)]

    def parts(k):
        l, j, n = jobs[k]
        own = (wg_ref, wu_ref, wd_ref)[n]
        other = (pg_ref, pu_ref, pd_ref)[n]
        new = (ng_ref, nu_ref, nd_ref)[n]
        buf = (wide if n == 2 else tall).at[k % DEPTH]
        return l, j, n, own, other, new, buf

    def load(k):
        l, j, n, own, other, new, buf = parts(k)
        mode, pos, starts = table[l, j]
        sem = in_sem.at[k % DEPTH]

        @pl.when(mode == KEEP)
        def _():
            pltpu.make_async_copy(own.at[l, j], buf, sem).start()

        @pl.when((mode == NEAR) & (pos < slots))
        def _():
            pltpu.make_async_copy(own.at[l, pos], buf, sem).start()

        @pl.when((mode == NEAR) & (pos >= slots))
        def _():
            pltpu.make_async_copy(other.at[l, pos - slots], buf, sem).start()

        @pl.when(mode == RINGED)
        def _():
            for side in range(2):
                start = starts[side] + 6 * n
                for source, owner in ((arr_ref, core), (far_ref, 1 - core)):
                    tall_at = 2 * TILE * (2 * owner + side)

                    @pl.loop(0, 6)
                    def _(t):
                        if n == 2:
                            r, c = TILE * (t // 2), tall_at + TILE * lax.rem(t, 2)
                        else:
                            r, c = tall_at + TILE * (t // 3), TILE * lax.rem(t, 3)
                        spot = (pl.ds(pl.multiple_of(r, TILE), TILE), pl.ds(pl.multiple_of(c, TILE), TILE))
                        pltpu.make_async_copy(source.at[l, side, start + t], buf.at[spot], sem).start()

    def arrive(k):
        l, j, n, own, other, new, buf = parts(k)
        pltpu.make_async_copy(own.at[l, j], buf, in_sem.at[k % DEPTH]).wait()

    def store(k):
        l, j, n, own, other, new, buf = parts(k)
        return pltpu.make_async_copy(buf, new.at[l, j], out_sem.at[k % DEPTH])

    ahead = DEPTH - 1
    for k in range(ahead):
        load(k)
    for k in range(len(jobs)):
        arrive(k)
        store(k).start()
        if k >= 1:
            store(k - 1).wait()
        if k + ahead < len(jobs):
            load(k + ahead)
    store(len(jobs) - 1).wait()


def run_place(group, old_map, move_slot, move_expert, w_gate, w_up, w_down, p_gate, p_up, p_down, arrived, far):
    layers, _, width, ffn = w_gate.shape
    any_spec = pl.BlockSpec(memory_space=pl.ANY)
    smem = pl.BlockSpec(memory_space=pltpu.SMEM)
    dma = pltpu.SemaphoreType.DMA
    return pl.pallas_call(
        functools.partial(place_kernel, group),
        name='place',
        out_shape=tuple(jax.ShapeDtypeStruct(w.shape, BF16) for w in (w_gate, w_up, w_down)) + (
            jax.ShapeDtypeStruct((layers,), jnp.int32),),
        in_specs=[smem] * 3 + [any_spec] * 8,
        out_specs=[any_spec] * 3 + [smem],
        scratch_shapes=[pltpu.VMEM((DEPTH, width, ffn), BF16), pltpu.VMEM((DEPTH, ffn, width), BF16), dma((DEPTH,)), dma((DEPTH,))],
        compiler_params=pltpu.CompilerParams(vmem_limit_bytes=48 * 2 ** 20),
    )(old_map, move_slot, move_expert, w_gate, w_up, w_down, p_gate, p_up, p_down, arrived, far)


def finish_moves(group, news, weights, over, old_map, move_slot, move_expert):
    layers, n_slots = old_map.shape
    slots = weights[0].shape[1]
    ring = [(d, (d + 1) % group) for d in range(group)]

    def one(k, news):
        me = lax.axis_index('ep')
        l = jnp.where(over[0] > 0, k, layers - 1)
        ids = jnp.arange(n_slots, dtype=jnp.int32)
        source = jnp.min(jnp.where(old_map[l] == move_expert[l, 1], ids, n_slots))
        here = source // slots == me
        there = move_slot[l, 1] // slots == me
        index = move_slot[l, 1] % slots
        own = tuple(w[l, source % slots] for w in weights)

        def hop(_, held):
            return tuple(jnp.where(here, o, lax.ppermute(h, 'ep', ring)) for o, h in zip(own, held))

        got = lax.fori_loop(0, group - 1, hop, own)
        return tuple(new.at[l, index].set(jnp.where(there, g, new[l, index])) for new, g in zip(news, got))

    return lax.fori_loop(0, jnp.sum(over), one, news)


def solution(mesh):
    group = mesh.shape['ep']

    def body(tok_in, routes, gate_vals, w_gate, w_up, w_down, sh_gate, sh_up, sh_down, old_map, move_slot, move_expert):
        maps = (old_map, move_slot, move_expert)
        by_choice = (routes.transpose(0, 2, 1), gate_vals.transpose(0, 2, 1))
        hidden, p_gate, p_up, p_down, arrived, far = run_moe(group, *maps, *by_choice, tok_in, w_gate, w_up, w_down, sh_gate, sh_up, sh_down)
        *news, over = run_place(group, *maps, w_gate, w_up, w_down, p_gate, p_up, p_down, arrived, far)
        news = finish_moves(group, tuple(news), (w_gate, w_up, w_down), over, *maps)
        return (hidden,) + tuple(news)

    weight_spec = P(None, TOKEN_AXES, None, None)
    route_spec = P(None, TOKEN_AXES, None)
    map_spec = P(None, 'replica')
    shared_spec = P(None, None, None)
    tok_spec = P(TOKEN_AXES, None)
    return jax.shard_map(body, mesh=mesh, in_specs=(tok_spec, route_spec, route_spec, weight_spec, weight_spec, weight_spec, shared_spec, shared_spec, shared_spec, map_spec, map_spec, map_spec), out_specs=(tok_spec, weight_spec, weight_spec, weight_spec), check_vma=False)
```

```python
import functools

import jax
import jax.numpy as jnp
from jax import lax
from jax.experimental import pallas as pl
from jax.experimental.pallas import tpu as pltpu
from jax.sharding import PartitionSpec as P

TOKEN_AXES = ('replica', 'ep')
MESH = pl.DeviceIdType.MESH
F32, BF16 = jnp.float32, jnp.bfloat16
CORES = 2
CHUNKS = 8
HALF = CHUNKS // 2
STEPS = 17
LANES = 128
TILE = 256
TILES = 18
LAG = 2
TICKS = TILES + 2 * LAG
RING = 6
PRE = {9: 2, 10: 2, 11: 2, 12: 2, 13: 3, 14: 3, 15: 4, 16: 4}


def read_plan(map_ref, slot_ref, expert_ref, l, chips, per_chip, chip, core, slots):
    def place_on(m, x):
        found = per_chip
        for a in reversed(range(per_chip)):
            found = jnp.where(map_ref[l, x * per_chip + a] == expert_ref[l, m], a, found)
        return found

    spots = [[place_on(m, x) for x in range(chips)] for m in range(2)]
    held = [[s < per_chip for s in row] for row in spots]
    goals = []
    for m in range(2):
        to = slot_ref[l, m]
        goal = 0
        for x in range(1, chips):
            goal = jnp.where(to >= x * per_chip, x, goal)
        goals.append(goal)

    def has(m, x):
        out = held[m][0] & (x == 0)
        for c in range(1, chips):
            out = out | (held[m][c] & (x == c))
        return out

    def lowest(m):
        out = chips - 1
        for c in reversed(range(chips - 1)):
            out = jnp.where(held[m][c], c, out)
        return out

    near = [has(m, goals[m]) for m in range(2)]
    neither = jnp.logical_not(near[0] | near[1])
    swap = neither & has(0, goals[1]) & has(1, goals[0])
    left_over = neither & jnp.logical_not(swap)
    origin = [jnp.where(near[m], goals[m], jnp.where(swap, goals[1 - m], lowest(m))) for m in range(2)]
    ringed = [jnp.logical_not(near[0]), jnp.logical_not(near[1] | left_over)]
    places = []
    for m in range(2):
        a = jnp.int32(0)
        for x in range(chips):
            a = jnp.where(chip == x, spots[m][x], a)
        mine = (a >= core * slots) & (a < (core + 1) * slots)
        places.append(jnp.where(mine, a - core * slots, slots + a - (1 - core) * slots))
    return goals, origin, near, ringed, left_over, places


def moe_kernel(group, map_ref, slot_ref, expert_ref, route_ref, gate_ref, tok_ref, wg_ref, wu_ref, wd_ref, sg_ref, su_ref, sd_ref,
               base_ref, first_ref, second_ref, pg_ref, pu_ref, pd_ref, arr_ref, far_ref,
               blk, part, rdir, rmrg, xin, wgb, wub, wdb, act, rbuf, gbuf, cbuf, ct, colb, pick, land, stage,
               ag_send, ag_recv, fw_send, fw_recv, co_send, co_recv, pw_send, pw_recv,
               di_send, di_recv, xi_send, xi_recv, mg_send, mg_recv, wg_sem, wu_sem, wd_sem, io_sem, out_sem, sum_sem,
               pick_sem, mv_send, mv_recv, arr_sem, far_send, far_recv):
    me = lax.axis_index('ep')
    core = lax.rem(me, CORES)
    chip = me // CORES
    right = lax.rem(me + CORES, group)
    left = lax.rem(me + group - CORES, group)
    mate = me + 1 - 2 * core
    rows_all, width = tok_ref.shape
    ffn = sg_ref.shape[2]
    layers = wg_ref.shape[0]
    slots = wg_ref.shape[1]
    piece = rows_all // CHUNKS
    half_rows = rows_all // 2
    total = layers * STEPS
    chips = group // CORES
    n_slots = group * slots

    def remote(src, dst, send, recv, dev):
        return pltpu.make_async_remote_copy(src_ref=src, dst_ref=dst, send_sem=send, recv_sem=recv,
                                            device_id={'ep': dev}, device_id_type=MESH)

    def rows(c):
        return pl.ds(pl.multiple_of(c * piece, piece), piece)

    def own_copy(side, c):
        late = c // HALF
        return remote(blk.at[0, rows(c)], blk.at[1 + late if side == 0 else 2 - late, rows(c)],
                      ag_send.at[side, c], ag_recv.at[side, c], right if side == 0 else left)

    def forward_copy(side, c):
        at = rows(c + side * HALF)
        return remote(blk.at[1, at], blk.at[3, at], fw_send.at[side, c], fw_recv.at[side, c],
                      right if side == 0 else left)

    def coef_copy(n):
        src, dst, dev = ((0, 1, right), (0, 2, left), (1, 3, right))[n]
        return remote(cbuf.at[src], cbuf.at[dst], co_send.at[n], co_recv.at[n], dev)

    def direct_copy(side, c):
        return remote(part.at[1, rows(c + side * HALF)], rdir.at[side, rows(c)], di_send.at[side, c],
                      di_recv.at[side, c], left if side == 0 else right)

    def relay_copy(side, c):
        return remote(part.at[3, rows(c + side * HALF)], xin.at[side, rows(c)], xi_send.at[side, c],
                      xi_recv.at[side, c], right if side == 0 else left)

    def merged_copy(side, c):
        return remote(part.at[2, rows(c + side * HALF)], rmrg.at[side, rows(c)], mg_send.at[side, c],
                      mg_recv.at[side, c], right if side == 0 else left)

    def sum_out(side, c):
        return pltpu.make_async_copy(part.at[2, rows(c + side * HALF)], (first_ref, second_ref)[side].at[rows(c)], sum_sem.at[side, c])

    def base_out(side, c):
        d = rows(c + side * HALF)
        return pltpu.make_async_copy(part.at[0, d], base_ref.at[d], out_sem.at[side, c])

    def mate_copies(l, j):
        return [remote(src.at[l, j], dst.at[l, j], pw_send.at[l, j, n], pw_recv.at[l, j, n], mate)
                for n, (src, dst) in enumerate(((wg_ref, pg_ref), (wu_ref, pu_ref), (wd_ref, pd_ref)))]

    def step_kind(i):
        late = i - 5
        turn = late // 4
        unit = jnp.where(i < 5, 0, jnp.where(turn == 0, 1, 4 - turn))
        pos = jnp.where(i < 5, jnp.where(i < 2, i, jnp.where(i == 2, 4, i - 1)), late - 4 * turn)
        kind = jnp.where(pos == 4, 2, jnp.where(pos < 2, 0, 1))
        return unit, kind, jnp.where(pos == 4, 0, lax.rem(pos, 2))

    def fetch(n, which):
        l = n // STEPS
        i = n - l * STEPS
        _, kind, slot = step_kind(i)
        buf = lax.rem(n, 2)

        def go(g, u, d):
            if which == 0:
                pltpu.make_async_copy(g, wgb.at[buf], wg_sem.at[buf]).start()
                pltpu.make_async_copy(u, wub.at[buf], wu_sem.at[buf]).start()
            else:
                pltpu.make_async_copy(d, wdb, wd_sem).start()

        @pl.when(kind == 0)
        def _():
            go(wg_ref.at[l, slot], wu_ref.at[l, slot], wd_ref.at[l, slot])

        @pl.when(kind == 1)
        def _():
            go(pg_ref.at[l, slot], pu_ref.at[l, slot], pd_ref.at[l, slot])

        @pl.when(kind == 2)
        def _():
            go(sg_ref.at[l], su_ref.at[l], sd_ref.at[l])

    def columns(u, first, second):
        mine = jnp.concatenate([cbuf[first, chip][:, :half_rows], cbuf[second, chip][:, half_rows:]], axis=1)
        full = jnp.concatenate([mine, jnp.zeros((LANES - mine.shape[0], rows_all), F32)], axis=0)
        ct[u] = full.T

    def picks(l, t, side):
        quarter = 2 * core + side
        at = lax.rem(t, 6)

        def pair(own, other, r, c):
            spot = (pl.ds(pl.multiple_of(r, TILE), TILE), pl.ds(pl.multiple_of(c, TILE), TILE))
            return (pltpu.make_async_copy(own.at[(l, slice(None)) + spot], pick.at[side, pl.ds(0, slots)], pick_sem.at[side, 0]),
                    pltpu.make_async_copy(other.at[(l, slice(None)) + spot], pick.at[side, pl.ds(slots, slots)], pick_sem.at[side, 1]))

        tall = 2 * TILE * quarter
        r3, c3 = at // 3, lax.rem(at, 3)
        r2, c2 = at // 2, lax.rem(at, 2)
        return (pair(wg_ref, pg_ref, tall + TILE * r3, TILE * c3), pair(wu_ref, pu_ref, tall + TILE * r3, TILE * c3),
                pair(wd_ref, pd_ref, TILE * r2, tall + TILE * c2))

    def pick_start(l, t):
        for side in range(2):
            for n, pair in enumerate(picks(l, t, side)):
                @pl.when(t // 6 == n)
                def _():
                    for copy in pair:
                        copy.start()

    def tile_copy(tick, side):
        return remote(stage.at[lax.rem(tick, 2), side], land.at[side, lax.rem(tick, RING)], mv_send.at[lax.rem(tick, 2), side],
                      mv_recv.at[side, lax.rem(tick, RING)], right if side == 0 else left)

    def tile_store(l, tick, side):
        return pltpu.make_async_copy(land.at[side, lax.rem(tick, RING)], arr_ref.at[l, side, tick], arr_sem.at[side, lax.rem(tick, 2)])

    def ring_step(l, tick):
        _, origin, _, ringed, _, places = read_plan(map_ref, slot_ref, expert_ref, l, chips, CORES * slots, chip, core, slots)
        sends = [ringed[m] & (origin[m] == chip) for m in range(2)]
        from_here = sends[0] | sends[1]
        place = jnp.where(sends[0], places[0], jnp.where(sends[1], places[1], 0))

        @pl.when(tick < TILES)
        def _():
            for side in range(2):
                for copy in picks(l, tick, side)[0]:
                    copy.wait()

        for side in range(2):
            @pl.when(tick >= 2)
            def _():
                tile_copy(tick - 2, side).wait_send()

            @pl.when(tick >= LAG)
            def _():
                tile_copy(tick - LAG, side).wait_recv()
                tile_store(l, tick - LAG, side).start()
                stage[lax.rem(tick, 2), side] = jnp.where(from_here, pick[side, place], land[side, lax.rem(tick + RING - LAG, RING)])

            @pl.when(tick < LAG)
            def _():
                stage[lax.rem(tick, 2), side] = pick[side, place]

        @pl.when(tick + 1 < TILES)
        def _():
            pick_start(l, tick + 1)

        for side in range(2):
            @pl.when(tick > LAG)
            def _():
                tile_store(l, tick - LAG - 1, side).wait()

            tile_copy(tick, side).start()

    def ring_finish(l):
        for side in range(2):
            tile_store(l, jnp.int32(TICKS - LAG - 1), side).wait()
            for tick in range(TICKS - LAG, TICKS):
                tile_copy(jnp.int32(tick), side).wait_recv()
                tile_store(l, jnp.int32(tick), side).start()
            for tick in range(TICKS - LAG, TICKS):
                tile_store(l, jnp.int32(tick), side).wait()
                tile_copy(jnp.int32(tick), side).wait_send()
        far_copy(l).start()

    def far_copy(l):
        return remote(arr_ref.at[l], far_ref.at[l], far_send.at[l], far_recv.at[l], mate)

    tok_in = pltpu.make_async_copy(tok_ref, blk.at[0], io_sem.at[0])
    route_in = pltpu.make_async_copy(route_ref, rbuf, io_sem.at[1])
    gate_in = pltpu.make_async_copy(gate_ref, gbuf, io_sem.at[2])
    tok_in.start()
    route_in.start()
    gate_in.start()
    fetch(jnp.int32(0), 0)
    fetch(jnp.int32(0), 1)

    barrier = pltpu.get_barrier_semaphore()
    for dev in (left, right, mate):
        pl.semaphore_signal(barrier, inc=1, device_id={'ep': dev}, device_id_type=MESH)
    pl.semaphore_wait(barrier, 3)

    tok_in.wait()
    for c in range(CHUNKS):
        own_copy(0, c).start()
        own_copy(1, (c + HALF) % CHUNKS).start()
    for l in range(layers):
        for j in range(slots):
            for copy in mate_copies(l, j):
                copy.start()

    route_in.wait()
    gate_in.wait()
    for l in range(layers):
        for q in range(n_slots):
            expert = map_ref[l, q]
            serves = jnp.float32(1.0)
            for p in range(q):
                serves = jnp.where(map_ref[l, p] == expert, 0.0, serves)
            gates = jnp.sum(jnp.where(rbuf[l] == expert, gbuf[l], 0.0), axis=0, keepdims=True)
            at = slots * CORES * l + q % (slots * CORES)
            cbuf[0, q // (slots * CORES), at:at + 1, :] = gates * serves
    coef_copy(0).start()
    coef_copy(1).start()
    columns(0, 0, 0)

    @pl.loop(0, layers)
    def layer(l):
        @pl.loop(0, STEPS)
        def step(i):
            n = l * STEPS + i
            unit, kind, slot = step_kind(i)
            buf = lax.rem(n, 2)

            for j, at in ((0, 2), (1, 3)):
                @pl.when(i == at)
                def _():
                    for copy in mate_copies(l, j):
                        copy.wait_recv()

            @pl.when(i == 4)
            def _():
                for c in range(HALF):
                    own_copy(0, c).wait_recv()
                    forward_copy(0, c).start()
                    own_copy(1, c + HALF).wait_recv()
                    forward_copy(1, c).start()
                pick_start(l, jnp.int32(0))

                @pl.when(l == 0)
                def _():
                    coef_copy(0).wait_recv()
                    coef_copy(2).start()
                    coef_copy(1).wait_recv()
                    columns(1, 1, 2)
                    columns(2, 2, 1)

            @pl.when(i == 9)
            def _():
                for c in range(HALF):
                    for side in range(2):
                        forward_copy(side, c).wait()

                @pl.when(l == 0)
                def _():
                    coef_copy(2).wait_recv()
                    columns(3, 3, 3)

            @pl.when(i == 13)
            def _():
                for c in range(HALF):
                    own_copy(0, c + HALF).wait_recv()
                    own_copy(1, c).wait_recv()

            for c in range(HALF):
                @pl.when(i == 9 + c)
                def _():
                    direct_copy(0, c).start()
                    direct_copy(1, c).start()

                @pl.when(i == 13 + c)
                def _():
                    relay_copy(0, c).start()
                    relay_copy(1, c).start()

            first, last = jnp.int32(0), jnp.int32(0)
            done = 0
            for at, count in sorted(PRE.items()):
                first = jnp.where(i == at, done, first)
                last = jnp.where(i == at, min(done + count, TICKS), last)
                done = min(done + count, TICKS)
            assert done == TICKS

            @pl.loop(first, last)
            def _(tick):
                ring_step(l, tick)

            pltpu.make_async_copy(wg_ref.at[0, 0], wgb.at[buf], wg_sem.at[buf]).wait()
            pltpu.make_async_copy(wu_ref.at[0, 0], wub.at[buf], wu_sem.at[buf]).wait()

            @pl.when(n + 1 < total)
            def _():
                fetch(n + 1, 0)

            place = 4 * l + jnp.where(kind == 0, 2 * core, 2 * (1 - core)) + slot
            lane = lax.broadcasted_iota(jnp.int32, (rows_all, LANES), 1)
            col = jnp.sum(jnp.where(lane == place, ct[unit], 0.0), axis=1, keepdims=True)
            col = jnp.where(kind == 2, 1.0, col)
            colb[...] = jnp.broadcast_to(col, (rows_all, LANES))

            @pl.when(i == 0)
            def _():
                part[0] = blk[0].astype(F32)

            @pl.when((i == 5) | (i == 9) | (i == 13))
            def _():
                part[unit] = jnp.zeros((rows_all, width), F32)

            @pl.loop(0, ffn // 256)
            def _(f):
                cols = pl.ds(pl.multiple_of(f * 256, 256), 256)
                gate = jnp.dot(blk[unit], wgb[buf, :, cols], preferred_element_type=F32)
                up = jnp.dot(blk[unit], wub[buf, :, cols], preferred_element_type=F32)
                act[:, cols] = (gate / (1.0 + jnp.exp(-gate)) * up).astype(BF16)

            pltpu.make_async_copy(wd_ref.at[0, 0], wdb, wd_sem).wait()

            @pl.loop(0, width // 512)
            def _(w):
                cols = pl.ds(pl.multiple_of(w * 512, 512), 512)
                down = jnp.dot(act[...], wdb[:, cols], preferred_element_type=F32)
                scale = jnp.concatenate([colb[...]] * 4, axis=1)
                part[unit, :, cols] = part[unit, :, cols] + scale * down

            @pl.when(n + 1 < total)
            def _():
                fetch(n + 1, 1)

        for c in range(CHUNKS):
            own_copy(0, c).wait_send()
            own_copy(1, c).wait_send()

        @pl.loop(0, HALF)
        def merge(c):
            for side in range(2):
                relay_copy(side, c).wait_recv()
                at = rows(c + side * HALF)
                part[2, at] = part[2, at] + xin[side, rows(c)]
            for side in range(2):
                @pl.when(l + 1 < layers)
                def _():
                    merged_copy(side, c).start()

                @pl.when(l + 1 == layers)
                def _():
                    sum_out(side, c).start()

        ring_finish(l)

        @pl.when(l + 1 < layers)
        def _():
            @pl.loop(0, HALF)
            def finish(c):
                for side in range(2):
                    direct_copy(side, c).wait_recv()
                    merged_copy(side, c).wait_recv()
                    d = c + side * HALF
                    blk[0, rows(d)] = (part[0, rows(d)] + rdir[side, rows(c)] + rmrg[side, rows(c)]).astype(BF16)
                for side in range(2):
                    own_copy(side, c + side * HALF).start()
                for side in range(2):
                    own_copy(1 - side, c + side * HALF).start()

            for c in range(HALF):
                for side in range(2):
                    merged_copy(side, c).wait_send()

        @pl.when(l + 1 == layers)
        def _():
            @pl.loop(0, HALF)
            def finish(c):
                for side in range(2):
                    direct_copy(side, c).wait_recv()
                    d = rows(c + side * HALF)
                    part[0, d] = part[0, d] + rdir[side, rows(c)]
                for side in range(2):
                    base_out(side, c).start()

        for c in range(HALF):
            for side in range(2):
                direct_copy(side, c).wait_send()
                relay_copy(side, c).wait_send()

    for c in range(HALF):
        for side in range(2):
            sum_out(side, c).wait()
            base_out(side, c).wait()
    for n in range(3):
        coef_copy(n).wait_send()
    for l in range(layers):
        far_copy(l).wait()
        for j in range(slots):
            for copy in mate_copies(l, j):
                copy.wait_send()


def run_moe(group, old_map, move_slot, move_expert, routes, gates, tok, w_gate, w_up, w_down, sh_gate, sh_up, sh_down):
    n_rows, width = tok.shape
    layers, slots, _, ffn = w_gate.shape
    half = n_rows // 2
    chips = group // CORES
    any_spec = pl.BlockSpec(memory_space=pl.ANY)
    dma = pltpu.SemaphoreType.DMA
    flops = 2 * n_rows * 3 * width * ffn * layers * STEPS
    arrivals = jax.ShapeDtypeStruct((layers, 2, TICKS, TILE, TILE), BF16)
    return pl.pallas_call(
        functools.partial(moe_kernel, group),
        name='moe',
        out_shape=(jax.ShapeDtypeStruct(tok.shape, F32),) + (jax.ShapeDtypeStruct((half, width), F32),) * 2 + tuple(
            jax.ShapeDtypeStruct(w.shape, BF16) for w in (w_gate, w_up, w_down)) + (arrivals, arrivals),
        in_specs=[pl.BlockSpec(memory_space=pltpu.SMEM)] * 3 + [any_spec] * 9,
        out_specs=[any_spec] * 8,
        scratch_shapes=[
            pltpu.VMEM((chips, n_rows, width), BF16),
            pltpu.VMEM((chips, n_rows, width), F32),
            pltpu.VMEM((2, half, width), F32),
            pltpu.VMEM((2, half, width), F32),
            pltpu.VMEM((2, half, width), F32),
            pltpu.VMEM((2, width, ffn), BF16),
            pltpu.VMEM((2, width, ffn), BF16),
            pltpu.VMEM((ffn, width), BF16),
            pltpu.VMEM((n_rows, ffn), BF16),
            pltpu.VMEM(routes.shape, jnp.int32),
            pltpu.VMEM(gates.shape, F32),
            pltpu.VMEM((chips, chips, layers * slots * CORES, n_rows), F32),
            pltpu.VMEM((chips, n_rows, LANES), F32),
            pltpu.VMEM((n_rows, LANES), F32),
            pltpu.VMEM((2, CORES * slots, TILE, TILE), BF16),
            pltpu.VMEM((2, RING, TILE, TILE), BF16),
            pltpu.VMEM((2, 2, TILE, TILE), BF16),
            dma((2, CHUNKS)), dma((2, CHUNKS)), dma((2, HALF)), dma((2, HALF)), dma((3,)), dma((3,)),
            dma((layers, slots, 3)), dma((layers, slots, 3)),
            dma((2, HALF)), dma((2, HALF)), dma((2, HALF)), dma((2, HALF)), dma((2, HALF)), dma((2, HALF)),
            dma((2,)), dma((2,)), dma, dma((3,)), dma((2, HALF)), dma((2, HALF)),
            dma((2, 2)), dma((2, 2)), dma((2, RING)), dma((2, 2)), dma((layers,)), dma((layers,)),
        ],
        compiler_params=pltpu.CompilerParams(collective_id=0, has_side_effects=True, vmem_limit_bytes=67043328),
        cost_estimate=pl.CostEstimate(flops=flops, bytes_accessed=400 * 2 ** 20, transcendentals=0),
    )(old_map, move_slot, move_expert, routes, gates, tok, w_gate, w_up, w_down, sh_gate, sh_up, sh_down)


KEEP, NEAR, RINGED = 0, 1, 2
DEPTH = 4


def place_kernel(group, map_ref, slot_ref, expert_ref, wg_ref, wu_ref, wd_ref, pg_ref, pu_ref, pd_ref, arr_ref, far_ref,
                 ng_ref, nu_ref, nd_ref, over_ref, tall, wide, in_sem, out_sem):
    layers, slots = wg_ref.shape[:2]
    me = lax.axis_index('ep')
    core = lax.rem(me, CORES)
    chip = me // CORES
    chips = group // CORES
    table = {}
    for l in range(layers):
        goals, origin, near, ringed, left_over, places = read_plan(map_ref, slot_ref, expert_ref, l, chips, CORES * slots, chip, core, slots)
        over_ref[l] = left_over.astype(jnp.int32)
        for j in range(slots):
            mode, pos, first, second = KEEP, 0, 0, 0
            for m in range(2):
                here = slot_ref[l, m] == me * slots + j
                ahead = lax.rem(goals[m] - origin[m] + chips, chips)
                mode = jnp.where(here, jnp.where(near[m], NEAR, jnp.where(ringed[m], RINGED, KEEP)), mode)
                pos = jnp.where(here, places[m], pos)
                first = jnp.where(here, (ahead - 1) * LAG, first)
                second = jnp.where(here, (chips - ahead - 1) * LAG, second)
            table[l, j] = mode, pos, (first, second)
    jobs = [(l, j, n) for l in range(layers) for j in range(slots) for n in range(3)]

    def parts(k):
        l, j, n = jobs[k]
        own = (wg_ref, wu_ref, wd_ref)[n]
        other = (pg_ref, pu_ref, pd_ref)[n]
        new = (ng_ref, nu_ref, nd_ref)[n]
        buf = (wide if n == 2 else tall).at[k % DEPTH]
        return l, j, n, own, other, new, buf

    def load(k):
        l, j, n, own, other, new, buf = parts(k)
        mode, pos, starts = table[l, j]
        sem = in_sem.at[k % DEPTH]

        @pl.when(mode == KEEP)
        def _():
            pltpu.make_async_copy(own.at[l, j], buf, sem).start()

        @pl.when((mode == NEAR) & (pos < slots))
        def _():
            pltpu.make_async_copy(own.at[l, pos], buf, sem).start()

        @pl.when((mode == NEAR) & (pos >= slots))
        def _():
            pltpu.make_async_copy(other.at[l, pos - slots], buf, sem).start()

        @pl.when(mode == RINGED)
        def _():
            for side in range(2):
                start = starts[side] + 6 * n
                for source, owner in ((arr_ref, core), (far_ref, 1 - core)):
                    tall_at = 2 * TILE * (2 * owner + side)

                    @pl.loop(0, 6)
                    def _(t):
                        if n == 2:
                            r, c = TILE * (t // 2), tall_at + TILE * lax.rem(t, 2)
                        else:
                            r, c = tall_at + TILE * (t // 3), TILE * lax.rem(t, 3)
                        spot = (pl.ds(pl.multiple_of(r, TILE), TILE), pl.ds(pl.multiple_of(c, TILE), TILE))
                        pltpu.make_async_copy(source.at[l, side, start + t], buf.at[spot], sem).start()

    def arrive(k):
        l, j, n, own, other, new, buf = parts(k)
        pltpu.make_async_copy(own.at[l, j], buf, in_sem.at[k % DEPTH]).wait()

    def store(k):
        l, j, n, own, other, new, buf = parts(k)
        return pltpu.make_async_copy(buf, new.at[l, j], out_sem.at[k % DEPTH])

    ahead = DEPTH - 1
    for k in range(ahead):
        load(k)
    for k in range(len(jobs)):
        arrive(k)
        store(k).start()
        if k >= 1:
            store(k - 1).wait()
        if k + ahead < len(jobs):
            load(k + ahead)
    store(len(jobs) - 1).wait()


def run_place(group, old_map, move_slot, move_expert, w_gate, w_up, w_down, p_gate, p_up, p_down, arrived, far):
    layers, _, width, ffn = w_gate.shape
    any_spec = pl.BlockSpec(memory_space=pl.ANY)
    smem = pl.BlockSpec(memory_space=pltpu.SMEM)
    dma = pltpu.SemaphoreType.DMA
    return pl.pallas_call(
        functools.partial(place_kernel, group),
        name='place',
        out_shape=tuple(jax.ShapeDtypeStruct(w.shape, BF16) for w in (w_gate, w_up, w_down)) + (
            jax.ShapeDtypeStruct((layers,), jnp.int32),),
        in_specs=[smem] * 3 + [any_spec] * 8,
        out_specs=[any_spec] * 3 + [smem],
        scratch_shapes=[pltpu.VMEM((DEPTH, width, ffn), BF16), pltpu.VMEM((DEPTH, ffn, width), BF16), dma((DEPTH,)), dma((DEPTH,))],
        compiler_params=pltpu.CompilerParams(vmem_limit_bytes=48 * 2 ** 20),
        cost_estimate=pl.CostEstimate(flops=2 * 10 ** 10, bytes_accessed=80 * 10 ** 6, transcendentals=0),
    )(old_map, move_slot, move_expert, w_gate, w_up, w_down, p_gate, p_up, p_down, arrived, far)


def finish_moves(group, news, weights, over, old_map, move_slot, move_expert):
    layers, n_slots = old_map.shape
    slots = weights[0].shape[1]
    ring = [(d, (d + 1) % group) for d in range(group)]

    def one(k, news):
        me = lax.axis_index('ep')
        l = jnp.where(over[0] > 0, k, layers - 1)
        ids = jnp.arange(n_slots, dtype=jnp.int32)
        source = jnp.min(jnp.where(old_map[l] == move_expert[l, 1], ids, n_slots))
        here = source // slots == me
        there = move_slot[l, 1] // slots == me
        index = move_slot[l, 1] % slots
        own = tuple(w[l, source % slots] for w in weights)

        def hop(_, held):
            return tuple(jnp.where(here, o, lax.ppermute(h, 'ep', ring)) for o, h in zip(own, held))

        got = lax.fori_loop(0, group - 1, hop, own)
        return tuple(new.at[l, index].set(jnp.where(there, g, new[l, index])) for new, g in zip(news, got))

    return lax.fori_loop(0, jnp.sum(over), one, news)


def solution(mesh):
    group = mesh.shape['ep']

    def body(tok_in, routes, gate_vals, w_gate, w_up, w_down, sh_gate, sh_up, sh_down, old_map, move_slot, move_expert):
        maps = (old_map, move_slot, move_expert)
        by_choice = (routes.transpose(0, 2, 1), gate_vals.transpose(0, 2, 1))
        base, first, second, p_gate, p_up, p_down, arrived, far = run_moe(group, *maps, *by_choice, tok_in, w_gate, w_up, w_down, sh_gate, sh_up, sh_down)
        *news, over = run_place(group, *maps, w_gate, w_up, w_down, p_gate, p_up, p_down, arrived, far)
        news = finish_moves(group, tuple(news), (w_gate, w_up, w_down), over, *maps)
        rightward = [(d, (d + CORES) % group) for d in range(group)]
        leftward = [(d, (d + group - CORES) % group) for d in range(group)]
        hidden = (base + jnp.concatenate([lax.ppermute(first, 'ep', rightward), lax.ppermute(second, 'ep', leftward)], axis=0)).astype(BF16)
        return (hidden,) + tuple(news)

    weight_spec = P(None, TOKEN_AXES, None, None)
    route_spec = P(None, TOKEN_AXES, None)
    map_spec = P(None, 'replica')
    shared_spec = P(None, None, None)
    tok_spec = P(TOKEN_AXES, None)
    return jax.shard_map(body, mesh=mesh, in_specs=(tok_spec, route_spec, route_spec, weight_spec, weight_spec, weight_spec, shared_spec, shared_spec, shared_spec, map_spec, map_spec, map_spec), out_specs=(tok_spec, weight_spec, weight_spec, weight_spec), check_vma=False)
```

```python
import functools

import jax
import jax.numpy as jnp
from jax import lax
from jax.experimental import pallas as pl
from jax.experimental.pallas import tpu as pltpu
from jax.sharding import PartitionSpec as P

TOKEN_AXES = ('replica', 'ep')
MESH = pl.DeviceIdType.MESH
F32, BF16 = jnp.float32, jnp.bfloat16
CORES = 2
CHUNKS = 8
HALF = CHUNKS // 2
STEPS = 17
LANES = 128
TILE = 256
TILES = 18
LAG = 2
TICKS = TILES + 2 * LAG
RING = 6
PRE = {9: 2, 10: 2, 11: 2, 12: 2, 13: 3, 14: 3, 15: 4, 16: 4}


def read_plan(map_ref, slot_ref, expert_ref, l, chips, per_chip, chip, core, slots):
    def place_on(m, x):
        found = per_chip
        for a in reversed(range(per_chip)):
            found = jnp.where(map_ref[l, x * per_chip + a] == expert_ref[l, m], a, found)
        return found

    spots = [[place_on(m, x) for x in range(chips)] for m in range(2)]
    held = [[s < per_chip for s in row] for row in spots]
    goals = []
    for m in range(2):
        to = slot_ref[l, m]
        goal = 0
        for x in range(1, chips):
            goal = jnp.where(to >= x * per_chip, x, goal)
        goals.append(goal)

    def has(m, x):
        out = held[m][0] & (x == 0)
        for c in range(1, chips):
            out = out | (held[m][c] & (x == c))
        return out

    def lowest(m):
        out = chips - 1
        for c in reversed(range(chips - 1)):
            out = jnp.where(held[m][c], c, out)
        return out

    near = [has(m, goals[m]) for m in range(2)]
    neither = jnp.logical_not(near[0] | near[1])
    swap = neither & has(0, goals[1]) & has(1, goals[0])
    left_over = neither & jnp.logical_not(swap)
    origin = [jnp.where(near[m], goals[m], jnp.where(swap, goals[1 - m], lowest(m))) for m in range(2)]
    ringed = [jnp.logical_not(near[0]), jnp.logical_not(near[1] | left_over)]
    places = []
    for m in range(2):
        a = jnp.int32(0)
        for x in range(chips):
            a = jnp.where(chip == x, spots[m][x], a)
        mine = (a >= core * slots) & (a < (core + 1) * slots)
        places.append(jnp.where(mine, a - core * slots, slots + a - (1 - core) * slots))
    return goals, origin, near, ringed, left_over, places


def moe_kernel(group, map_ref, slot_ref, expert_ref, route_ref, gate_ref, tok_ref, wg_ref, wu_ref, wd_ref, sg_ref, su_ref, sd_ref,
               base_ref, first_ref, second_ref, pg_ref, pu_ref, pd_ref, arr_ref, far_ref,
               blk, part, rdir, rmrg, xin, wgb, wub, wdb, act, rbuf, gbuf, cbuf, ct, colb, pick, land, stage,
               ag_send, ag_recv, fw_send, fw_recv, co_send, co_recv, pw_send, pw_recv,
               di_send, di_recv, xi_send, xi_recv, mg_send, mg_recv, wg_sem, wu_sem, wd_sem, io_sem, out_sem, sum_sem,
               pick_sem, mv_send, mv_recv, arr_sem, far_send, far_recv):
    me = lax.axis_index('ep')
    core = lax.rem(me, CORES)
    chip = me // CORES
    right = lax.rem(me + CORES, group)
    left = lax.rem(me + group - CORES, group)
    mate = me + 1 - 2 * core
    rows_all, width = tok_ref.shape
    ffn = sg_ref.shape[2]
    layers = wg_ref.shape[0]
    slots = wg_ref.shape[1]
    piece = rows_all // CHUNKS
    half_rows = rows_all // 2
    total = layers * STEPS
    chips = group // CORES
    n_slots = group * slots

    def remote(src, dst, send, recv, dev):
        return pltpu.make_async_remote_copy(src_ref=src, dst_ref=dst, send_sem=send, recv_sem=recv,
                                            device_id={'ep': dev}, device_id_type=MESH)

    def rows(c):
        return pl.ds(pl.multiple_of(c * piece, piece), piece)

    def own_copy(side, c):
        late = c // HALF
        return remote(blk.at[0, rows(c)], blk.at[1 + late if side == 0 else 2 - late, rows(c)],
                      ag_send.at[side, c], ag_recv.at[side, c], right if side == 0 else left)

    def forward_copy(side, c):
        at = rows(c + side * HALF)
        return remote(blk.at[1, at], blk.at[3, at], fw_send.at[side, c], fw_recv.at[side, c],
                      right if side == 0 else left)

    def coef_copy(n):
        src, dst, dev = ((0, 1, right), (0, 2, left), (1, 3, right))[n]
        return remote(cbuf.at[src], cbuf.at[dst], co_send.at[n], co_recv.at[n], dev)

    def direct_copy(side, c):
        return remote(part.at[1, rows(c + side * HALF)], rdir.at[side, rows(c)], di_send.at[side, c],
                      di_recv.at[side, c], left if side == 0 else right)

    def relay_copy(side, c):
        return remote(part.at[3, rows(c + side * HALF)], xin.at[side, rows(c)], xi_send.at[side, c],
                      xi_recv.at[side, c], right if side == 0 else left)

    def merged_copy(side, c):
        return remote(part.at[2, rows(c + side * HALF)], rmrg.at[side, rows(c)], mg_send.at[side, c],
                      mg_recv.at[side, c], right if side == 0 else left)

    def sum_out(side, c):
        return pltpu.make_async_copy(part.at[2, rows(c + side * HALF)], (first_ref, second_ref)[side].at[rows(c)], sum_sem.at[side, c])

    def base_out(side, c):
        d = rows(c + side * HALF)
        return pltpu.make_async_copy(part.at[0, d], base_ref.at[d], out_sem.at[side, c])

    def mate_copies(l, j):
        return [remote(src.at[l, j], dst.at[l, j], pw_send.at[l, j, n], pw_recv.at[l, j, n], mate)
                for n, (src, dst) in enumerate(((wg_ref, pg_ref), (wu_ref, pu_ref), (wd_ref, pd_ref)))]

    def step_kind(i):
        late = i - 5
        turn = late // 4
        unit = jnp.where(i < 5, 0, jnp.where(turn == 0, 1, 4 - turn))
        pos = jnp.where(i < 5, jnp.where(i < 2, i, jnp.where(i == 2, 4, i - 1)), late - 4 * turn)
        kind = jnp.where(pos == 4, 2, jnp.where(pos < 2, 0, 1))
        return unit, kind, jnp.where(pos == 4, 0, lax.rem(pos, 2))

    def fetch(n, which):
        l = n // STEPS
        i = n - l * STEPS
        _, kind, slot = step_kind(i)
        buf = lax.rem(n, 2)

        def go(g, u, d):
            if which == 0:
                pltpu.make_async_copy(g, wgb.at[buf], wg_sem.at[buf]).start()
                pltpu.make_async_copy(u, wub.at[buf], wu_sem.at[buf]).start()
            else:
                pltpu.make_async_copy(d, wdb, wd_sem).start()

        @pl.when(kind == 0)
        def _():
            go(wg_ref.at[l, slot], wu_ref.at[l, slot], wd_ref.at[l, slot])

        @pl.when(kind == 1)
        def _():
            go(pg_ref.at[l, slot], pu_ref.at[l, slot], pd_ref.at[l, slot])

        @pl.when(kind == 2)
        def _():
            go(sg_ref.at[l], su_ref.at[l], sd_ref.at[l])

    def columns(u, first, second):
        mine = jnp.concatenate([cbuf[first, chip][:, :half_rows], cbuf[second, chip][:, half_rows:]], axis=1)
        full = jnp.concatenate([mine, jnp.zeros((LANES - mine.shape[0], rows_all), F32)], axis=0)
        ct[u] = full.T

    def picks(l, t, side):
        quarter = 2 * core + side
        at = lax.rem(t, 6)

        def pair(own, other, r, c):
            spot = (pl.ds(pl.multiple_of(r, TILE), TILE), pl.ds(pl.multiple_of(c, TILE), TILE))
            return (pltpu.make_async_copy(own.at[(l, slice(None)) + spot], pick.at[side, pl.ds(0, slots)], pick_sem.at[side, 0]),
                    pltpu.make_async_copy(other.at[(l, slice(None)) + spot], pick.at[side, pl.ds(slots, slots)], pick_sem.at[side, 1]))

        tall = 2 * TILE * quarter
        r3, c3 = at // 3, lax.rem(at, 3)
        r2, c2 = at // 2, lax.rem(at, 2)
        return (pair(wg_ref, pg_ref, tall + TILE * r3, TILE * c3), pair(wu_ref, pu_ref, tall + TILE * r3, TILE * c3),
                pair(wd_ref, pd_ref, TILE * r2, tall + TILE * c2))

    def pick_start(l, t):
        for side in range(2):
            for n, pair in enumerate(picks(l, t, side)):
                @pl.when(t // 6 == n)
                def _():
                    for copy in pair:
                        copy.start()

    def tile_copy(tick, side):
        return remote(stage.at[lax.rem(tick, 2), side], land.at[side, lax.rem(tick, RING)], mv_send.at[lax.rem(tick, 2), side],
                      mv_recv.at[side, lax.rem(tick, RING)], right if side == 0 else left)

    def tile_out(l, tick, side, begin):
        tile = land.at[side, lax.rem(tick, RING)]
        turn = lax.rem(tick, 2)
        keep = pltpu.make_async_copy(tile, arr_ref.at[l, side, tick], arr_sem.at[side, turn])
        give = remote(tile, far_ref.at[l, side, tick], far_send.at[side, turn], far_recv.at[l], mate)
        if begin:
            keep.start()
            give.start()
        else:
            keep.wait()
            give.wait_send()

    def ring_step(l, tick):
        _, origin, _, ringed, _, places = read_plan(map_ref, slot_ref, expert_ref, l, chips, CORES * slots, chip, core, slots)
        sends = [ringed[m] & (origin[m] == chip) for m in range(2)]
        from_here = sends[0] | sends[1]
        place = jnp.where(sends[0], places[0], jnp.where(sends[1], places[1], 0))

        @pl.when(tick < TILES)
        def _():
            for side in range(2):
                for copy in picks(l, tick, side)[0]:
                    copy.wait()

        for side in range(2):
            @pl.when(tick >= 2)
            def _():
                tile_copy(tick - 2, side).wait_send()

            @pl.when(tick >= LAG)
            def _():
                tile_copy(tick - LAG, side).wait_recv()
                tile_out(l, tick - LAG, side, True)
                stage[lax.rem(tick, 2), side] = jnp.where(from_here, pick[side, place], land[side, lax.rem(tick + RING - LAG, RING)])

            @pl.when(tick < LAG)
            def _():
                stage[lax.rem(tick, 2), side] = pick[side, place]

        @pl.when(tick + 1 < TILES)
        def _():
            pick_start(l, tick + 1)

        for side in range(2):
            @pl.when(tick > LAG)
            def _():
                tile_out(l, tick - LAG - 1, side, False)

            tile_copy(tick, side).start()

    def ring_finish(l):
        for side in range(2):
            tile_out(l, jnp.int32(TICKS - LAG - 1), side, False)
            for tick in range(TICKS - LAG, TICKS):
                tile_copy(jnp.int32(tick), side).wait_recv()
                tile_out(l, jnp.int32(tick), side, True)
            for tick in range(TICKS - LAG, TICKS):
                tile_out(l, jnp.int32(tick), side, False)
                tile_copy(jnp.int32(tick), side).wait_send()

    tok_in = pltpu.make_async_copy(tok_ref, blk.at[0], io_sem.at[0])
    route_in = pltpu.make_async_copy(route_ref, rbuf, io_sem.at[1])
    gate_in = pltpu.make_async_copy(gate_ref, gbuf, io_sem.at[2])
    tok_in.start()
    route_in.start()
    gate_in.start()
    fetch(jnp.int32(0), 0)
    fetch(jnp.int32(0), 1)

    barrier = pltpu.get_barrier_semaphore()
    for dev in (left, right, mate):
        pl.semaphore_signal(barrier, inc=1, device_id={'ep': dev}, device_id_type=MESH)
    pl.semaphore_wait(barrier, 3)

    tok_in.wait()
    for c in range(CHUNKS):
        own_copy(0, c).start()
        own_copy(1, (c + HALF) % CHUNKS).start()
    for l in range(layers):
        for j in range(slots):
            for copy in mate_copies(l, j):
                copy.start()

    route_in.wait()
    gate_in.wait()
    for l in range(layers):
        for q in range(n_slots):
            expert = map_ref[l, q]
            serves = jnp.float32(1.0)
            for p in range(q):
                serves = jnp.where(map_ref[l, p] == expert, 0.0, serves)
            gates = jnp.sum(jnp.where(rbuf[l] == expert, gbuf[l], 0.0), axis=0, keepdims=True)
            at = slots * CORES * l + q % (slots * CORES)
            cbuf[0, q // (slots * CORES), at:at + 1, :] = gates * serves
    coef_copy(0).start()
    coef_copy(1).start()
    columns(0, 0, 0)

    @pl.loop(0, layers)
    def layer(l):
        @pl.loop(0, STEPS)
        def step(i):
            n = l * STEPS + i
            unit, kind, slot = step_kind(i)
            buf = lax.rem(n, 2)

            for j, at in ((0, 2), (1, 3)):
                @pl.when(i == at)
                def _():
                    for copy in mate_copies(l, j):
                        copy.wait_recv()

            @pl.when(i == 4)
            def _():
                for c in range(HALF):
                    own_copy(0, c).wait_recv()
                    forward_copy(0, c).start()
                    own_copy(1, c + HALF).wait_recv()
                    forward_copy(1, c).start()
                pick_start(l, jnp.int32(0))

                @pl.when(l == 0)
                def _():
                    coef_copy(0).wait_recv()
                    coef_copy(2).start()
                    coef_copy(1).wait_recv()
                    columns(1, 1, 2)
                    columns(2, 2, 1)

            @pl.when(i == 9)
            def _():
                for c in range(HALF):
                    for side in range(2):
                        forward_copy(side, c).wait()

                @pl.when(l == 0)
                def _():
                    coef_copy(2).wait_recv()
                    columns(3, 3, 3)

            @pl.when(i == 13)
            def _():
                for c in range(HALF):
                    own_copy(0, c + HALF).wait_recv()
                    own_copy(1, c).wait_recv()

            for c in range(HALF):
                @pl.when(i == 9 + c)
                def _():
                    direct_copy(0, c).start()
                    direct_copy(1, c).start()

                @pl.when(i == 13 + c)
                def _():
                    relay_copy(0, c).start()
                    relay_copy(1, c).start()

            first, last = jnp.int32(0), jnp.int32(0)
            done = 0
            for at, count in sorted(PRE.items()):
                first = jnp.where(i == at, done, first)
                last = jnp.where(i == at, min(done + count, TICKS), last)
                done = min(done + count, TICKS)
            assert done == TICKS

            @pl.loop(first, last)
            def _(tick):
                ring_step(l, tick)

            pltpu.make_async_copy(wg_ref.at[0, 0], wgb.at[buf], wg_sem.at[buf]).wait()
            pltpu.make_async_copy(wu_ref.at[0, 0], wub.at[buf], wu_sem.at[buf]).wait()

            @pl.when(n + 1 < total)
            def _():
                fetch(n + 1, 0)

            place = 4 * l + jnp.where(kind == 0, 2 * core, 2 * (1 - core)) + slot
            lane = lax.broadcasted_iota(jnp.int32, (rows_all, LANES), 1)
            col = jnp.sum(jnp.where(lane == place, ct[unit], 0.0), axis=1, keepdims=True)
            col = jnp.where(kind == 2, 1.0, col)
            colb[...] = jnp.broadcast_to(col, (rows_all, LANES))

            @pl.when(i == 0)
            def _():
                part[0] = blk[0].astype(F32)

            @pl.when((i == 5) | (i == 9) | (i == 13))
            def _():
                part[unit] = jnp.zeros((rows_all, width), F32)

            @pl.loop(0, ffn // 256)
            def _(f):
                cols = pl.ds(pl.multiple_of(f * 256, 256), 256)
                gate = jnp.dot(blk[unit], wgb[buf, :, cols], preferred_element_type=F32)
                up = jnp.dot(blk[unit], wub[buf, :, cols], preferred_element_type=F32)
                act[:, cols] = (gate / (1.0 + jnp.exp(-gate)) * up).astype(BF16)

            pltpu.make_async_copy(wd_ref.at[0, 0], wdb, wd_sem).wait()

            @pl.loop(0, width // 512)
            def _(w):
                cols = pl.ds(pl.multiple_of(w * 512, 512), 512)
                down = jnp.dot(act[...], wdb[:, cols], preferred_element_type=F32)
                scale = jnp.concatenate([colb[...]] * 4, axis=1)
                part[unit, :, cols] = part[unit, :, cols] + scale * down

            @pl.when(n + 1 < total)
            def _():
                fetch(n + 1, 1)

        for c in range(CHUNKS):
            own_copy(0, c).wait_send()
            own_copy(1, c).wait_send()

        @pl.loop(0, HALF)
        def merge(c):
            for side in range(2):
                relay_copy(side, c).wait_recv()
                at = rows(c + side * HALF)
                part[2, at] = part[2, at] + xin[side, rows(c)]
            for side in range(2):
                @pl.when(l + 1 < layers)
                def _():
                    merged_copy(side, c).start()

                @pl.when(l + 1 == layers)
                def _():
                    sum_out(side, c).start()

        ring_finish(l)

        @pl.when(l + 1 < layers)
        def _():
            @pl.loop(0, HALF)
            def finish(c):
                for side in range(2):
                    direct_copy(side, c).wait_recv()
                    merged_copy(side, c).wait_recv()
                    d = c + side * HALF
                    blk[0, rows(d)] = (part[0, rows(d)] + rdir[side, rows(c)] + rmrg[side, rows(c)]).astype(BF16)
                for side in range(2):
                    own_copy(side, c + side * HALF).start()
                for side in range(2):
                    own_copy(1 - side, c + side * HALF).start()

            for c in range(HALF):
                for side in range(2):
                    merged_copy(side, c).wait_send()

        @pl.when(l + 1 == layers)
        def _():
            @pl.loop(0, HALF)
            def finish(c):
                for side in range(2):
                    direct_copy(side, c).wait_recv()
                    d = rows(c + side * HALF)
                    part[0, d] = part[0, d] + rdir[side, rows(c)]
                for side in range(2):
                    base_out(side, c).start()

        for c in range(HALF):
            for side in range(2):
                direct_copy(side, c).wait_send()
                relay_copy(side, c).wait_send()

    for c in range(HALF):
        for side in range(2):
            sum_out(side, c).wait()
            base_out(side, c).wait()
    for n in range(3):
        coef_copy(n).wait_send()
    for l in range(layers):
        pltpu.make_async_copy(arr_ref.at[l], far_ref.at[l], far_recv.at[l]).wait()
        for j in range(slots):
            for copy in mate_copies(l, j):
                copy.wait_send()


def run_moe(group, old_map, move_slot, move_expert, routes, gates, tok, w_gate, w_up, w_down, sh_gate, sh_up, sh_down):
    n_rows, width = tok.shape
    layers, slots, _, ffn = w_gate.shape
    half = n_rows // 2
    chips = group // CORES
    any_spec = pl.BlockSpec(memory_space=pl.ANY)
    dma = pltpu.SemaphoreType.DMA
    flops = 2 * n_rows * 3 * width * ffn * layers * STEPS
    arrivals = jax.ShapeDtypeStruct((layers, 2, TICKS, TILE, TILE), BF16)
    return pl.pallas_call(
        functools.partial(moe_kernel, group),
        name='moe',
        out_shape=(jax.ShapeDtypeStruct(tok.shape, F32),) + (jax.ShapeDtypeStruct((half, width), F32),) * 2 + tuple(
            jax.ShapeDtypeStruct(w.shape, BF16) for w in (w_gate, w_up, w_down)) + (arrivals, arrivals),
        in_specs=[pl.BlockSpec(memory_space=pltpu.SMEM)] * 3 + [any_spec] * 9,
        out_specs=[any_spec] * 8,
        scratch_shapes=[
            pltpu.VMEM((chips, n_rows, width), BF16),
            pltpu.VMEM((chips, n_rows, width), F32),
            pltpu.VMEM((2, half, width), F32),
            pltpu.VMEM((2, half, width), F32),
            pltpu.VMEM((2, half, width), F32),
            pltpu.VMEM((2, width, ffn), BF16),
            pltpu.VMEM((2, width, ffn), BF16),
            pltpu.VMEM((ffn, width), BF16),
            pltpu.VMEM((n_rows, ffn), BF16),
            pltpu.VMEM(routes.shape, jnp.int32),
            pltpu.VMEM(gates.shape, F32),
            pltpu.VMEM((chips, chips, layers * slots * CORES, n_rows), F32),
            pltpu.VMEM((chips, n_rows, LANES), F32),
            pltpu.VMEM((n_rows, LANES), F32),
            pltpu.VMEM((2, CORES * slots, TILE, TILE), BF16),
            pltpu.VMEM((2, RING, TILE, TILE), BF16),
            pltpu.VMEM((2, 2, TILE, TILE), BF16),
            dma((2, CHUNKS)), dma((2, CHUNKS)), dma((2, HALF)), dma((2, HALF)), dma((3,)), dma((3,)),
            dma((layers, slots, 3)), dma((layers, slots, 3)),
            dma((2, HALF)), dma((2, HALF)), dma((2, HALF)), dma((2, HALF)), dma((2, HALF)), dma((2, HALF)),
            dma((2,)), dma((2,)), dma, dma((3,)), dma((2, HALF)), dma((2, HALF)),
            dma((2, 2)), dma((2, 2)), dma((2, RING)), dma((2, 2)), dma((2, 2)), dma((layers,)),
        ],
        compiler_params=pltpu.CompilerParams(collective_id=0, has_side_effects=True, vmem_limit_bytes=67043328),
        cost_estimate=pl.CostEstimate(flops=flops, bytes_accessed=400 * 2 ** 20, transcendentals=0),
    )(old_map, move_slot, move_expert, routes, gates, tok, w_gate, w_up, w_down, sh_gate, sh_up, sh_down)


KEEP, NEAR, RINGED = 0, 1, 2
DEPTH = 4


def place_kernel(group, map_ref, slot_ref, expert_ref, wg_ref, wu_ref, wd_ref, pg_ref, pu_ref, pd_ref, arr_ref, far_ref,
                 ng_ref, nu_ref, nd_ref, over_ref, tall, wide, in_sem, out_sem):
    layers, slots = wg_ref.shape[:2]
    me = lax.axis_index('ep')
    core = lax.rem(me, CORES)
    chip = me // CORES
    chips = group // CORES
    table = {}
    for l in range(layers):
        goals, origin, near, ringed, left_over, places = read_plan(map_ref, slot_ref, expert_ref, l, chips, CORES * slots, chip, core, slots)
        over_ref[l] = left_over.astype(jnp.int32)
        for j in range(slots):
            mode, pos, first, second = KEEP, 0, 0, 0
            for m in range(2):
                here = slot_ref[l, m] == me * slots + j
                ahead = lax.rem(goals[m] - origin[m] + chips, chips)
                mode = jnp.where(here, jnp.where(near[m], NEAR, jnp.where(ringed[m], RINGED, KEEP)), mode)
                pos = jnp.where(here, places[m], pos)
                first = jnp.where(here, (ahead - 1) * LAG, first)
                second = jnp.where(here, (chips - ahead - 1) * LAG, second)
            table[l, j] = mode, pos, (first, second)
    jobs = [(l, j, n) for l in range(layers) for j in range(slots) for n in range(3)]

    def parts(k):
        l, j, n = jobs[k]
        own = (wg_ref, wu_ref, wd_ref)[n]
        other = (pg_ref, pu_ref, pd_ref)[n]
        new = (ng_ref, nu_ref, nd_ref)[n]
        buf = (wide if n == 2 else tall).at[k % DEPTH]
        return l, j, n, own, other, new, buf

    def load(k):
        l, j, n, own, other, new, buf = parts(k)
        mode, pos, starts = table[l, j]
        sem = in_sem.at[k % DEPTH]

        @pl.when(mode == KEEP)
        def _():
            pltpu.make_async_copy(own.at[l, j], buf, sem).start()

        @pl.when((mode == NEAR) & (pos < slots))
        def _():
            pltpu.make_async_copy(own.at[l, pos], buf, sem).start()

        @pl.when((mode == NEAR) & (pos >= slots))
        def _():
            pltpu.make_async_copy(other.at[l, pos - slots], buf, sem).start()

        @pl.when(mode == RINGED)
        def _():
            for side in range(2):
                start = starts[side] + 6 * n
                for source, owner in ((arr_ref, core), (far_ref, 1 - core)):
                    tall_at = 2 * TILE * (2 * owner + side)

                    @pl.loop(0, 6)
                    def _(t):
                        if n == 2:
                            r, c = TILE * (t // 2), tall_at + TILE * lax.rem(t, 2)
                        else:
                            r, c = tall_at + TILE * (t // 3), TILE * lax.rem(t, 3)
                        spot = (pl.ds(pl.multiple_of(r, TILE), TILE), pl.ds(pl.multiple_of(c, TILE), TILE))
                        pltpu.make_async_copy(source.at[l, side, start + t], buf.at[spot], sem).start()

    def arrive(k):
        l, j, n, own, other, new, buf = parts(k)
        pltpu.make_async_copy(own.at[l, j], buf, in_sem.at[k % DEPTH]).wait()

    def store(k):
        l, j, n, own, other, new, buf = parts(k)
        return pltpu.make_async_copy(buf, new.at[l, j], out_sem.at[k % DEPTH])

    ahead = DEPTH - 1
    for k in range(ahead):
        load(k)
    for k in range(len(jobs)):
        arrive(k)
        store(k).start()
        if k >= 1:
            store(k - 1).wait()
        if k + ahead < len(jobs):
            load(k + ahead)
    store(len(jobs) - 1).wait()


def run_place(group, old_map, move_slot, move_expert, w_gate, w_up, w_down, p_gate, p_up, p_down, arrived, far):
    layers, _, width, ffn = w_gate.shape
    any_spec = pl.BlockSpec(memory_space=pl.ANY)
    smem = pl.BlockSpec(memory_space=pltpu.SMEM)
    dma = pltpu.SemaphoreType.DMA
    return pl.pallas_call(
        functools.partial(place_kernel, group),
        name='place',
        out_shape=tuple(jax.ShapeDtypeStruct(w.shape, BF16) for w in (w_gate, w_up, w_down)) + (
            jax.ShapeDtypeStruct((layers,), jnp.int32),),
        in_specs=[smem] * 3 + [any_spec] * 8,
        out_specs=[any_spec] * 3 + [smem],
        scratch_shapes=[pltpu.VMEM((DEPTH, width, ffn), BF16), pltpu.VMEM((DEPTH, ffn, width), BF16), dma((DEPTH,)), dma((DEPTH,))],
        compiler_params=pltpu.CompilerParams(vmem_limit_bytes=48 * 2 ** 20),
        cost_estimate=pl.CostEstimate(flops=2 * 10 ** 10, bytes_accessed=80 * 10 ** 6, transcendentals=0),
    )(old_map, move_slot, move_expert, w_gate, w_up, w_down, p_gate, p_up, p_down, arrived, far)


def finish_moves(group, news, weights, over, old_map, move_slot, move_expert):
    layers, n_slots = old_map.shape
    slots = weights[0].shape[1]
    ring = [(d, (d + 1) % group) for d in range(group)]

    def one(k, news):
        me = lax.axis_index('ep')
        l = jnp.where(over[0] > 0, k, layers - 1)
        ids = jnp.arange(n_slots, dtype=jnp.int32)
        source = jnp.min(jnp.where(old_map[l] == move_expert[l, 1], ids, n_slots))
        here = source // slots == me
        there = move_slot[l, 1] // slots == me
        index = move_slot[l, 1] % slots
        own = tuple(w[l, source % slots] for w in weights)

        def hop(_, held):
            return tuple(jnp.where(here, o, lax.ppermute(h, 'ep', ring)) for o, h in zip(own, held))

        got = lax.fori_loop(0, group - 1, hop, own)
        return tuple(new.at[l, index].set(jnp.where(there, g, new[l, index])) for new, g in zip(news, got))

    return lax.fori_loop(0, jnp.sum(over), one, news)


def solution(mesh):
    group = mesh.shape['ep']

    def body(tok_in, routes, gate_vals, w_gate, w_up, w_down, sh_gate, sh_up, sh_down, old_map, move_slot, move_expert):
        maps = (old_map, move_slot, move_expert)
        by_choice = (routes.transpose(0, 2, 1), gate_vals.transpose(0, 2, 1))
        base, first, second, p_gate, p_up, p_down, arrived, far = run_moe(group, *maps, *by_choice, tok_in, w_gate, w_up, w_down, sh_gate, sh_up, sh_down)
        *news, over = run_place(group, *maps, w_gate, w_up, w_down, p_gate, p_up, p_down, arrived, far)
        news = finish_moves(group, tuple(news), (w_gate, w_up, w_down), over, *maps)
        rightward = [(d, (d + CORES) % group) for d in range(group)]
        leftward = [(d, (d + group - CORES) % group) for d in range(group)]
        hidden = (base + jnp.concatenate([lax.ppermute(first, 'ep', rightward), lax.ppermute(second, 'ep', leftward)], axis=0)).astype(BF16)
        return (hidden,) + tuple(news)

    weight_spec = P(None, TOKEN_AXES, None, None)
    route_spec = P(None, TOKEN_AXES, None)
    map_spec = P(None, 'replica')
    shared_spec = P(None, None, None)
    tok_spec = P(TOKEN_AXES, None)
    return jax.shard_map(body, mesh=mesh, in_specs=(tok_spec, route_spec, route_spec, weight_spec, weight_spec, weight_spec, shared_spec, shared_spec, shared_spec, map_spec, map_spec, map_spec), out_specs=(tok_spec, weight_spec, weight_spec, weight_spec), check_vma=False)
```

```python
import functools

import jax
import jax.numpy as jnp
from jax import lax
from jax.experimental import pallas as pl
from jax.experimental.pallas import tpu as pltpu
from jax.sharding import PartitionSpec as P

TOKEN_AXES = ('replica', 'ep')
MESH = pl.DeviceIdType.MESH
F32, BF16 = jnp.float32, jnp.bfloat16
CORES = 2
CHUNKS = 8
HALF = CHUNKS // 2
STEPS = 17
LANES = 128
TILE = 256
TILES = 18
LAG = 1
TICKS = TILES + 2 * LAG
RING = 4
PIECES = 8
FIRST = 5


def read_plan(map_ref, slot_ref, expert_ref, l, chips, per_chip, chip, core, slots):
    def place_on(m, x):
        found = per_chip
        for a in reversed(range(per_chip)):
            found = jnp.where(map_ref[l, x * per_chip + a] == expert_ref[l, m], a, found)
        return found

    spots = [[place_on(m, x) for x in range(chips)] for m in range(2)]
    held = [[s < per_chip for s in row] for row in spots]
    goals = []
    for m in range(2):
        to = slot_ref[l, m]
        goal = 0
        for x in range(1, chips):
            goal = jnp.where(to >= x * per_chip, x, goal)
        goals.append(goal)

    def has(m, x):
        out = held[m][0] & (x == 0)
        for c in range(1, chips):
            out = out | (held[m][c] & (x == c))
        return out

    def lowest(m):
        out = chips - 1
        for c in reversed(range(chips - 1)):
            out = jnp.where(held[m][c], c, out)
        return out

    near = [has(m, goals[m]) for m in range(2)]
    neither = jnp.logical_not(near[0] | near[1])
    swap = neither & has(0, goals[1]) & has(1, goals[0])
    left_over = neither & jnp.logical_not(swap)
    origin = [jnp.where(near[m], goals[m], jnp.where(swap, goals[1 - m], lowest(m))) for m in range(2)]
    ringed = [jnp.logical_not(near[0]), jnp.logical_not(near[1] | left_over)]
    places = []
    for m in range(2):
        a = jnp.int32(0)
        for x in range(chips):
            a = jnp.where(chip == x, spots[m][x], a)
        mine = (a >= core * slots) & (a < (core + 1) * slots)
        places.append(jnp.where(mine, a - core * slots, slots + a - (1 - core) * slots))
    return goals, origin, near, ringed, left_over, places


def moe_kernel(group, map_ref, slot_ref, expert_ref, route_ref, gate_ref, tok_ref, wg_ref, wu_ref, wd_ref, sg_ref, su_ref, sd_ref,
               base_ref, first_ref, second_ref, pg_ref, pu_ref, pd_ref, arr_ref, far_ref,
               blk, part, rdir, rmrg, xin, wgb, wub, wdb, act, rbuf, gbuf, cbuf, ct, colb, pick, land, stage,
               ag_send, ag_recv, fw_send, fw_recv, co_send, co_recv, pw_send, pw_recv,
               di_send, di_recv, xi_send, xi_recv, mg_send, mg_recv, wg_sem, wu_sem, wd_sem, io_sem, out_sem, sum_sem,
               pick_sem, mv_send, mv_recv, arr_sem, far_send, far_recv):
    me = lax.axis_index('ep')
    core = lax.rem(me, CORES)
    chip = me // CORES
    right = lax.rem(me + CORES, group)
    left = lax.rem(me + group - CORES, group)
    mate = me + 1 - 2 * core
    rows_all, width = tok_ref.shape
    ffn = sg_ref.shape[2]
    layers = wg_ref.shape[0]
    slots = wg_ref.shape[1]
    piece = rows_all // CHUNKS
    half_rows = rows_all // 2
    total = layers * STEPS
    chips = group // CORES
    n_slots = group * slots

    def remote(src, dst, send, recv, dev):
        return pltpu.make_async_remote_copy(src_ref=src, dst_ref=dst, send_sem=send, recv_sem=recv,
                                            device_id={'ep': dev}, device_id_type=MESH)

    def rows(c):
        return pl.ds(pl.multiple_of(c * piece, piece), piece)

    def sums(c):
        size = half_rows // PIECES
        return pl.ds(pl.multiple_of(c * size, size), size)

    def own_copy(side, c):
        late = c // HALF
        return remote(blk.at[0, rows(c)], blk.at[1 + late if side == 0 else 2 - late, rows(c)],
                      ag_send.at[side, c], ag_recv.at[side, c], right if side == 0 else left)

    def forward_copy(side, c):
        at = rows(c + side * HALF)
        return remote(blk.at[1, at], blk.at[3, at], fw_send.at[side, c], fw_recv.at[side, c],
                      right if side == 0 else left)

    def coef_copy(n):
        src, dst, dev = ((0, 1, right), (0, 2, left), (1, 3, right))[n]
        return remote(cbuf.at[src], cbuf.at[dst], co_send.at[n], co_recv.at[n], dev)

    def direct_copy(side, c):
        return remote(part.at[1, sums(c + side * PIECES)], rdir.at[side, sums(c)], di_send.at[side, c],
                      di_recv.at[side, c], left if side == 0 else right)

    def relay_copy(side, c):
        return remote(part.at[3, sums(c + side * PIECES)], xin.at[side, sums(c)], xi_send.at[side, c],
                      xi_recv.at[side, c], right if side == 0 else left)

    def merged_copy(side, c):
        return remote(part.at[2, sums(c + side * PIECES)], rmrg.at[side, sums(c)], mg_send.at[side, c],
                      mg_recv.at[side, c], right if side == 0 else left)

    def sum_out(side, c):
        return pltpu.make_async_copy(part.at[2, sums(c + side * PIECES)], (first_ref, second_ref)[side].at[sums(c)], sum_sem.at[side, c])

    def base_out(side, c):
        d = sums(c + side * PIECES)
        return pltpu.make_async_copy(part.at[0, d], base_ref.at[d], out_sem.at[side, c])

    def mate_copies(l, j):
        return [remote(src.at[l, j], dst.at[l, j], pw_send.at[l, j, n], pw_recv.at[l, j, n], mate)
                for n, (src, dst) in enumerate(((wg_ref, pg_ref), (wu_ref, pu_ref), (wd_ref, pd_ref)))]

    def step_kind(i):
        late = i - 5
        turn = late // 4
        unit = jnp.where(i < 5, 0, jnp.where(turn == 0, 1, 4 - turn))
        pos = jnp.where(i < 5, jnp.where(i < 2, i, jnp.where(i == 2, 4, i - 1)), late - 4 * turn)
        kind = jnp.where(pos == 4, 2, jnp.where(pos < 2, 0, 1))
        return unit, kind, jnp.where(pos == 4, 0, lax.rem(pos, 2))

    def fetch(n, which):
        l = n // STEPS
        i = n - l * STEPS
        _, kind, slot = step_kind(i)
        buf = lax.rem(n, 2)

        def go(g, u, d):
            if which == 0:
                pltpu.make_async_copy(g, wgb.at[buf], wg_sem.at[buf]).start()
                pltpu.make_async_copy(u, wub.at[buf], wu_sem.at[buf]).start()
            else:
                pltpu.make_async_copy(d, wdb, wd_sem).start()

        @pl.when(kind == 0)
        def _():
            go(wg_ref.at[l, slot], wu_ref.at[l, slot], wd_ref.at[l, slot])

        @pl.when(kind == 1)
        def _():
            go(pg_ref.at[l, slot], pu_ref.at[l, slot], pd_ref.at[l, slot])

        @pl.when(kind == 2)
        def _():
            go(sg_ref.at[l], su_ref.at[l], sd_ref.at[l])

    def columns(u, first, second):
        mine = jnp.concatenate([cbuf[first, chip][:, :half_rows], cbuf[second, chip][:, half_rows:]], axis=1)
        full = jnp.concatenate([mine, jnp.zeros((LANES - mine.shape[0], rows_all), F32)], axis=0)
        ct[u] = full.T

    def picks(l, t, side):
        quarter = 2 * core + side
        at = lax.rem(t, 6)

        def pair(own, other, r, c):
            spot = (pl.ds(pl.multiple_of(r, TILE), TILE), pl.ds(pl.multiple_of(c, TILE), TILE))
            return (pltpu.make_async_copy(own.at[(l, slice(None)) + spot], pick.at[side, pl.ds(0, slots)], pick_sem.at[side, 0]),
                    pltpu.make_async_copy(other.at[(l, slice(None)) + spot], pick.at[side, pl.ds(slots, slots)], pick_sem.at[side, 1]))

        tall = 2 * TILE * quarter
        r3, c3 = at // 3, lax.rem(at, 3)
        r2, c2 = at // 2, lax.rem(at, 2)
        return (pair(wg_ref, pg_ref, tall + TILE * r3, TILE * c3), pair(wu_ref, pu_ref, tall + TILE * r3, TILE * c3),
                pair(wd_ref, pd_ref, TILE * r2, tall + TILE * c2))

    def pick_start(l, t):
        for side in range(2):
            for n, pair in enumerate(picks(l, t, side)):
                @pl.when(t // 6 == n)
                def _():
                    for copy in pair:
                        copy.start()

    def tile_copy(tick, side):
        return remote(stage.at[lax.rem(tick, 2), side], land.at[side, lax.rem(tick, RING)], mv_send.at[lax.rem(tick, 2), side],
                      mv_recv.at[side, lax.rem(tick, RING)], right if side == 0 else left)

    def tile_out(l, tick, side, begin):
        tile = land.at[side, lax.rem(tick, RING)]
        turn = lax.rem(tick, 2)
        keep = pltpu.make_async_copy(tile, arr_ref.at[l, side, tick], arr_sem.at[side, turn])
        give = remote(tile, far_ref.at[l, side, tick], far_send.at[side, turn], far_recv.at[l], mate)
        if begin:
            keep.start()
            give.start()
        else:
            keep.wait()
            give.wait_send()

    def ring_step(l, tick):
        _, origin, _, ringed, _, places = read_plan(map_ref, slot_ref, expert_ref, l, chips, CORES * slots, chip, core, slots)
        sends = [ringed[m] & (origin[m] == chip) for m in range(2)]
        from_here = sends[0] | sends[1]
        place = jnp.where(sends[0], places[0], jnp.where(sends[1], places[1], 0))

        @pl.when(tick < TILES)
        def _():
            for side in range(2):
                for copy in picks(l, tick, side)[0]:
                    copy.wait()

        for side in range(2):
            @pl.when(tick >= 2)
            def _():
                tile_copy(tick - 2, side).wait_send()

            @pl.when(tick >= LAG)
            def _():
                tile_copy(tick - LAG, side).wait_recv()
                tile_out(l, tick - LAG, side, True)
                stage[lax.rem(tick, 2), side] = jnp.where(from_here, pick[side, place], land[side, lax.rem(tick + RING - LAG, RING)])

            @pl.when(tick < LAG)
            def _():
                stage[lax.rem(tick, 2), side] = pick[side, place]

        @pl.when(tick + 1 < TILES)
        def _():
            pick_start(l, tick + 1)

        for side in range(2):
            @pl.when(tick > LAG)
            def _():
                tile_out(l, tick - LAG - 1, side, False)

            tile_copy(tick, side).start()

    def beat(l, k):
        ring_step(l, k)

        @pl.when(k < HALF)
        def _():
            own_copy(0, k + HALF).start()
            own_copy(1, k).start()

        @pl.when((k >= HALF) & (k < HALF + PIECES))
        def _():
            direct_copy(0, k - HALF).start()
            direct_copy(1, k - HALF).start()

        @pl.when(k >= HALF + PIECES)
        def _():
            relay_copy(0, k - HALF - PIECES).start()
            relay_copy(1, k - HALF - PIECES).start()

    def ring_finish(l):
        for side in range(2):
            tile_out(l, jnp.int32(TICKS - LAG - 1), side, False)
            for tick in range(TICKS - LAG, TICKS):
                tile_copy(jnp.int32(tick), side).wait_recv()
                tile_out(l, jnp.int32(tick), side, True)
            for tick in range(TICKS - LAG, TICKS):
                tile_out(l, jnp.int32(tick), side, False)
            for tick in range(TICKS - 2, TICKS):
                tile_copy(jnp.int32(tick), side).wait_send()

    tok_in = pltpu.make_async_copy(tok_ref, blk.at[0], io_sem.at[0])
    route_in = pltpu.make_async_copy(route_ref, rbuf, io_sem.at[1])
    gate_in = pltpu.make_async_copy(gate_ref, gbuf, io_sem.at[2])
    tok_in.start()
    route_in.start()
    gate_in.start()
    fetch(jnp.int32(0), 0)
    fetch(jnp.int32(0), 1)

    barrier = pltpu.get_barrier_semaphore()
    for dev in (left, right, mate):
        pl.semaphore_signal(barrier, inc=1, device_id={'ep': dev}, device_id_type=MESH)
    pl.semaphore_wait(barrier, 3)

    tok_in.wait()
    for c in range(HALF):
        own_copy(0, c).start()
        own_copy(1, c + HALF).start()
    for l in range(layers):
        for j in range(slots):
            for copy in mate_copies(l, j):
                copy.start()

    route_in.wait()
    gate_in.wait()
    for l in range(layers):
        for q in range(n_slots):
            expert = map_ref[l, q]
            serves = jnp.float32(1.0)
            for p in range(q):
                serves = jnp.where(map_ref[l, p] == expert, 0.0, serves)
            gates = jnp.sum(jnp.where(rbuf[l] == expert, gbuf[l], 0.0), axis=0, keepdims=True)
            at = slots * CORES * l + q % (slots * CORES)
            cbuf[0, q // (slots * CORES), at:at + 1, :] = gates * serves
    coef_copy(0).start()
    coef_copy(1).start()
    columns(0, 0, 0)

    @pl.loop(0, layers)
    def layer(l):
        @pl.loop(0, STEPS)
        def step(i):
            n = l * STEPS + i
            unit, kind, slot = step_kind(i)
            buf = lax.rem(n, 2)

            for j, at in ((0, 2), (1, 3)):
                @pl.when(i == at)
                def _():
                    for copy in mate_copies(l, j):
                        copy.wait_recv()

            for at, pieces in ((2, (0,)), (3, (1, 2)), (4, (3,))):
                @pl.when(i == at)
                def _():
                    for c in pieces:
                        own_copy(0, c).wait_recv()
                        forward_copy(0, c).start()
                        own_copy(1, c + HALF).wait_recv()
                        forward_copy(1, c).start()

            @pl.when(i == 4)
            def _():
                pick_start(l, jnp.int32(0))

                @pl.when(l == 0)
                def _():
                    coef_copy(0).wait_recv()
                    coef_copy(2).start()
                    coef_copy(1).wait_recv()
                    columns(1, 1, 2)
                    columns(2, 2, 1)

            @pl.when(i == 9)
            def _():
                for c in range(HALF):
                    for side in range(2):
                        forward_copy(side, c).wait()

                @pl.when(l == 0)
                def _():
                    coef_copy(2).wait_recv()
                    columns(3, 3, 3)

            @pl.when(i == 13)
            def _():
                for c in range(HALF):
                    own_copy(0, c + HALF).wait_recv()
                    own_copy(1, c).wait_recv()

            tick = jnp.where(i < FIRST + HALF, i - FIRST, HALF + 2 * (i - FIRST - HALF))

            @pl.when(i >= FIRST)
            def _():
                beat(l, tick)

            pltpu.make_async_copy(wg_ref.at[0, 0], wgb.at[buf], wg_sem.at[buf]).wait()
            pltpu.make_async_copy(wu_ref.at[0, 0], wub.at[buf], wu_sem.at[buf]).wait()

            @pl.when(n + 1 < total)
            def _():
                fetch(n + 1, 0)

            place = 4 * l + jnp.where(kind == 0, 2 * core, 2 * (1 - core)) + slot
            lane = lax.broadcasted_iota(jnp.int32, (rows_all, LANES), 1)
            col = jnp.sum(jnp.where(lane == place, ct[unit], 0.0), axis=1, keepdims=True)
            col = jnp.where(kind == 2, 1.0, col)
            colb[...] = jnp.broadcast_to(col, (rows_all, LANES))

            @pl.when(i == 0)
            def _():
                part[0] = blk[0].astype(F32)

            @pl.when((i == 5) | (i == 9) | (i == 13))
            def _():
                part[unit] = jnp.zeros((rows_all, width), F32)

            @pl.loop(0, ffn // 256)
            def _(f):
                cols = pl.ds(pl.multiple_of(f * 256, 256), 256)
                gate = jnp.dot(blk[unit], wgb[buf, :, cols], preferred_element_type=F32)
                up = jnp.dot(blk[unit], wub[buf, :, cols], preferred_element_type=F32)
                act[:, cols] = (gate / (1.0 + jnp.exp(-gate)) * up).astype(BF16)

            @pl.when(i >= FIRST + HALF)
            def _():
                beat(l, tick + 1)

            pltpu.make_async_copy(wd_ref.at[0, 0], wdb, wd_sem).wait()

            @pl.loop(0, width // 512)
            def _(w):
                cols = pl.ds(pl.multiple_of(w * 512, 512), 512)
                down = jnp.dot(act[...], wdb[:, cols], preferred_element_type=F32)
                scale = jnp.concatenate([colb[...]] * 4, axis=1)
                part[unit, :, cols] = part[unit, :, cols] + scale * down

            @pl.when(n + 1 < total)
            def _():
                fetch(n + 1, 1)

        for c in range(CHUNKS):
            own_copy(0, c).wait_send()
            own_copy(1, c).wait_send()

        @pl.loop(0, PIECES)
        def merge(c):
            for side in range(2):
                relay_copy(side, c).wait_recv()
                at = sums(c + side * PIECES)
                part[2, at] = part[2, at] + xin[side, sums(c)]
            for side in range(2):
                @pl.when(l + 1 < layers)
                def _():
                    merged_copy(side, c).start()

                @pl.when(l + 1 == layers)
                def _():
                    sum_out(side, c).start()

        ring_finish(l)

        @pl.when(l + 1 < layers)
        def _():
            @pl.loop(0, HALF)
            def finish(c):
                for side in range(2):
                    for p in range(PIECES // HALF):
                        direct_copy(side, c * (PIECES // HALF) + p).wait_recv()
                        merged_copy(side, c * (PIECES // HALF) + p).wait_recv()
                    d = rows(c + side * HALF)
                    blk[0, d] = (part[0, d] + rdir[side, rows(c)] + rmrg[side, rows(c)]).astype(BF16)
                for side in range(2):
                    own_copy(side, c + side * HALF).start()

            for c in range(PIECES):
                for side in range(2):
                    merged_copy(side, c).wait_send()

        @pl.when(l + 1 == layers)
        def _():
            @pl.loop(0, PIECES)
            def finish(c):
                for side in range(2):
                    direct_copy(side, c).wait_recv()
                    d = sums(c + side * PIECES)
                    part[0, d] = part[0, d] + rdir[side, sums(c)]
                for side in range(2):
                    base_out(side, c).start()

        for c in range(PIECES):
            for side in range(2):
                direct_copy(side, c).wait_send()
                relay_copy(side, c).wait_send()

    for c in range(PIECES):
        for side in range(2):
            sum_out(side, c).wait()
            base_out(side, c).wait()
    for n in range(3):
        coef_copy(n).wait_send()
    for l in range(layers):
        pltpu.make_async_copy(arr_ref.at[l], far_ref.at[l], far_recv.at[l]).wait()
        for j in range(slots):
            for copy in mate_copies(l, j):
                copy.wait_send()


def run_moe(group, old_map, move_slot, move_expert, routes, gates, tok, w_gate, w_up, w_down, sh_gate, sh_up, sh_down):
    n_rows, width = tok.shape
    layers, slots, _, ffn = w_gate.shape
    half = n_rows // 2
    chips = group // CORES
    any_spec = pl.BlockSpec(memory_space=pl.ANY)
    dma = pltpu.SemaphoreType.DMA
    flops = 2 * n_rows * 3 * width * ffn * layers * STEPS
    arrivals = jax.ShapeDtypeStruct((layers, 2, TICKS, TILE, TILE), BF16)
    return pl.pallas_call(
        functools.partial(moe_kernel, group),
        name='moe',
        out_shape=(jax.ShapeDtypeStruct(tok.shape, F32),) + (jax.ShapeDtypeStruct((half, width), F32),) * 2 + tuple(
            jax.ShapeDtypeStruct(w.shape, BF16) for w in (w_gate, w_up, w_down)) + (arrivals, arrivals),
        in_specs=[pl.BlockSpec(memory_space=pltpu.SMEM)] * 3 + [any_spec] * 9,
        out_specs=[any_spec] * 8,
        scratch_shapes=[
            pltpu.VMEM((chips, n_rows, width), BF16),
            pltpu.VMEM((chips, n_rows, width), F32),
            pltpu.VMEM((2, half, width), F32),
            pltpu.VMEM((2, half, width), F32),
            pltpu.VMEM((2, half, width), F32),
            pltpu.VMEM((2, width, ffn), BF16),
            pltpu.VMEM((2, width, ffn), BF16),
            pltpu.VMEM((ffn, width), BF16),
            pltpu.VMEM((n_rows, ffn), BF16),
            pltpu.VMEM(routes.shape, jnp.int32),
            pltpu.VMEM(gates.shape, F32),
            pltpu.VMEM((chips, chips, layers * slots * CORES, n_rows), F32),
            pltpu.VMEM((chips, n_rows, LANES), F32),
            pltpu.VMEM((n_rows, LANES), F32),
            pltpu.VMEM((2, CORES * slots, TILE, TILE), BF16),
            pltpu.VMEM((2, RING, TILE, TILE), BF16),
            pltpu.VMEM((2, 2, TILE, TILE), BF16),
            dma((2, CHUNKS)), dma((2, CHUNKS)), dma((2, HALF)), dma((2, HALF)), dma((3,)), dma((3,)),
            dma((layers, slots, 3)), dma((layers, slots, 3)),
            dma((2, PIECES)), dma((2, PIECES)), dma((2, PIECES)), dma((2, PIECES)), dma((2, PIECES)), dma((2, PIECES)),
            dma((2,)), dma((2,)), dma, dma((3,)), dma((2, PIECES)), dma((2, PIECES)),
            dma((2, 2)), dma((2, 2)), dma((2, RING)), dma((2, 2)), dma((2, 2)), dma((layers,)),
        ],
        compiler_params=pltpu.CompilerParams(collective_id=0, has_side_effects=True, vmem_limit_bytes=67043328),
        cost_estimate=pl.CostEstimate(flops=flops, bytes_accessed=400 * 2 ** 20, transcendentals=0),
    )(old_map, move_slot, move_expert, routes, gates, tok, w_gate, w_up, w_down, sh_gate, sh_up, sh_down)


KEEP, NEAR, RINGED = 0, 1, 2
DEPTH = 4


def place_kernel(group, map_ref, slot_ref, expert_ref, wg_ref, wu_ref, wd_ref, pg_ref, pu_ref, pd_ref, arr_ref, far_ref,
                 ng_ref, nu_ref, nd_ref, over_ref, tall, wide, in_sem, out_sem):
    layers, slots = wg_ref.shape[:2]
    me = lax.axis_index('ep')
    core = lax.rem(me, CORES)
    chip = me // CORES
    chips = group // CORES
    table = {}
    for l in range(layers):
        goals, origin, near, ringed, left_over, places = read_plan(map_ref, slot_ref, expert_ref, l, chips, CORES * slots, chip, core, slots)
        over_ref[l] = left_over.astype(jnp.int32)
        for j in range(slots):
            mode, pos, first, second = KEEP, 0, 0, 0
            for m in range(2):
                here = slot_ref[l, m] == me * slots + j
                ahead = lax.rem(goals[m] - origin[m] + chips, chips)
                mode = jnp.where(here, jnp.where(near[m], NEAR, jnp.where(ringed[m], RINGED, KEEP)), mode)
                pos = jnp.where(here, places[m], pos)
                first = jnp.where(here, (ahead - 1) * LAG, first)
                second = jnp.where(here, (chips - ahead - 1) * LAG, second)
            table[l, j] = mode, pos, (first, second)
    jobs = [(l, j, n) for l in range(layers) for j in range(slots) for n in range(3)]

    def parts(k):
        l, j, n = jobs[k]
        own = (wg_ref, wu_ref, wd_ref)[n]
        other = (pg_ref, pu_ref, pd_ref)[n]
        new = (ng_ref, nu_ref, nd_ref)[n]
        buf = (wide if n == 2 else tall).at[k % DEPTH]
        return l, j, n, own, other, new, buf

    def load(k):
        l, j, n, own, other, new, buf = parts(k)
        mode, pos, starts = table[l, j]
        sem = in_sem.at[k % DEPTH]

        @pl.when(mode == KEEP)
        def _():
            pltpu.make_async_copy(own.at[l, j], buf, sem).start()

        @pl.when((mode == NEAR) & (pos < slots))
        def _():
            pltpu.make_async_copy(own.at[l, pos], buf, sem).start()

        @pl.when((mode == NEAR) & (pos >= slots))
        def _():
            pltpu.make_async_copy(other.at[l, pos - slots], buf, sem).start()

        @pl.when(mode == RINGED)
        def _():
            for side in range(2):
                start = starts[side] + 6 * n
                for source, owner in ((arr_ref, core), (far_ref, 1 - core)):
                    tall_at = 2 * TILE * (2 * owner + side)

                    @pl.loop(0, 6)
                    def _(t):
                        if n == 2:
                            r, c = TILE * (t // 2), tall_at + TILE * lax.rem(t, 2)
                        else:
                            r, c = tall_at + TILE * (t // 3), TILE * lax.rem(t, 3)
                        spot = (pl.ds(pl.multiple_of(r, TILE), TILE), pl.ds(pl.multiple_of(c, TILE), TILE))
                        pltpu.make_async_copy(source.at[l, side, start + t], buf.at[spot], sem).start()

    def arrive(k):
        l, j, n, own, other, new, buf = parts(k)
        pltpu.make_async_copy(own.at[l, j], buf, in_sem.at[k % DEPTH]).wait()

    def store(k):
        l, j, n, own, other, new, buf = parts(k)
        return pltpu.make_async_copy(buf, new.at[l, j], out_sem.at[k % DEPTH])

    ahead = DEPTH - 1
    for k in range(ahead):
        load(k)
    for k in range(len(jobs)):
        arrive(k)
        store(k).start()
        if k >= 1:
            store(k - 1).wait()
        if k + ahead < len(jobs):
            load(k + ahead)
    store(len(jobs) - 1).wait()


def run_place(group, old_map, move_slot, move_expert, w_gate, w_up, w_down, p_gate, p_up, p_down, arrived, far):
    layers, _, width, ffn = w_gate.shape
    any_spec = pl.BlockSpec(memory_space=pl.ANY)
    smem = pl.BlockSpec(memory_space=pltpu.SMEM)
    dma = pltpu.SemaphoreType.DMA
    return pl.pallas_call(
        functools.partial(place_kernel, group),
        name='place',
        out_shape=tuple(jax.ShapeDtypeStruct(w.shape, BF16) for w in (w_gate, w_up, w_down)) + (
            jax.ShapeDtypeStruct((layers,), jnp.int32),),
        in_specs=[smem] * 3 + [any_spec] * 8,
        out_specs=[any_spec] * 3 + [smem],
        scratch_shapes=[pltpu.VMEM((DEPTH, width, ffn), BF16), pltpu.VMEM((DEPTH, ffn, width), BF16), dma((DEPTH,)), dma((DEPTH,))],
        compiler_params=pltpu.CompilerParams(vmem_limit_bytes=48 * 2 ** 20),
        cost_estimate=pl.CostEstimate(flops=2 * 10 ** 10, bytes_accessed=80 * 10 ** 6, transcendentals=0),
    )(old_map, move_slot, move_expert, w_gate, w_up, w_down, p_gate, p_up, p_down, arrived, far)


def finish_moves(group, news, weights, over, old_map, move_slot, move_expert):
    layers, n_slots = old_map.shape
    slots = weights[0].shape[1]
    ring = [(d, (d + 1) % group) for d in range(group)]

    def one(k, news):
        me = lax.axis_index('ep')
        l = jnp.where(over[0] > 0, k, layers - 1)
        ids = jnp.arange(n_slots, dtype=jnp.int32)
        source = jnp.min(jnp.where(old_map[l] == move_expert[l, 1], ids, n_slots))
        here = source // slots == me
        there = move_slot[l, 1] // slots == me
        index = move_slot[l, 1] % slots
        own = tuple(w[l, source % slots] for w in weights)

        def hop(_, held):
            return tuple(jnp.where(here, o, lax.ppermute(h, 'ep', ring)) for o, h in zip(own, held))

        got = lax.fori_loop(0, group - 1, hop, own)
        return tuple(new.at[l, index].set(jnp.where(there, g, new[l, index])) for new, g in zip(news, got))

    return lax.fori_loop(0, jnp.sum(over), one, news)


def solution(mesh):
    group = mesh.shape['ep']

    def body(tok_in, routes, gate_vals, w_gate, w_up, w_down, sh_gate, sh_up, sh_down, old_map, move_slot, move_expert):
        maps = (old_map, move_slot, move_expert)
        by_choice = (routes.transpose(0, 2, 1), gate_vals.transpose(0, 2, 1))
        base, first, second, p_gate, p_up, p_down, arrived, far = run_moe(group, *maps, *by_choice, tok_in, w_gate, w_up, w_down, sh_gate, sh_up, sh_down)
        *news, over = run_place(group, *maps, w_gate, w_up, w_down, p_gate, p_up, p_down, arrived, far)
        news = finish_moves(group, tuple(news), (w_gate, w_up, w_down), over, *maps)
        rightward = [(d, (d + CORES) % group) for d in range(group)]
        leftward = [(d, (d + group - CORES) % group) for d in range(group)]
        hidden = (base + jnp.concatenate([lax.ppermute(first, 'ep', rightward), lax.ppermute(second, 'ep', leftward)], axis=0)).astype(BF16)
        return (hidden,) + tuple(news)

    weight_spec = P(None, TOKEN_AXES, None, None)
    route_spec = P(None, TOKEN_AXES, None)
    map_spec = P(None, 'replica')
    shared_spec = P(None, None, None)
    tok_spec = P(TOKEN_AXES, None)
    return jax.shard_map(body, mesh=mesh, in_specs=(tok_spec, route_spec, route_spec, weight_spec, weight_spec, weight_spec, shared_spec, shared_spec, shared_spec, map_spec, map_spec, map_spec), out_specs=(tok_spec, weight_spec, weight_spec, weight_spec), check_vma=False)
```

```python
import functools

import jax
import jax.numpy as jnp
from jax import lax
from jax.experimental import pallas as pl
from jax.experimental.pallas import tpu as pltpu
from jax.sharding import PartitionSpec as P

TOKEN_AXES = ('replica', 'ep')
MESH = pl.DeviceIdType.MESH
F32, BF16 = jnp.float32, jnp.bfloat16
CORES = 2
CHUNKS = 8
HALF = CHUNKS // 2
STEPS = 17
LANES = 128
TILE = 256
TILES = 36
PER = TILES // 3
TICKS = TILES // 2 + 1
RING = 4
PIECES = 8
EARLY = 5
FIRST = 5


def read_plan(map_ref, slot_ref, expert_ref, l, chips, per_chip, chip, core, slots):
    def place_on(m, x):
        found = per_chip
        for a in reversed(range(per_chip)):
            found = jnp.where(map_ref[l, x * per_chip + a] == expert_ref[l, m], a, found)
        return found

    spots = [[place_on(m, x) for x in range(chips)] for m in range(2)]
    held = [[s < per_chip for s in row] for row in spots]
    goals = []
    for m in range(2):
        to = slot_ref[l, m]
        goal = 0
        for x in range(1, chips):
            goal = jnp.where(to >= x * per_chip, x, goal)
        goals.append(goal)

    def has(m, x):
        out = held[m][0] & (x == 0)
        for c in range(1, chips):
            out = out | (held[m][c] & (x == c))
        return out

    def lowest(m):
        out = chips - 1
        for c in reversed(range(chips - 1)):
            out = jnp.where(held[m][c], c, out)
        return out

    near = [has(m, goals[m]) for m in range(2)]
    neither = jnp.logical_not(near[0] | near[1])
    swap = neither & has(0, goals[1]) & has(1, goals[0])
    left_over = neither & jnp.logical_not(swap)
    origin = [jnp.where(near[m], goals[m], jnp.where(swap, goals[1 - m], lowest(m))) for m in range(2)]
    ringed = [jnp.logical_not(near[0]), jnp.logical_not(near[1] | left_over)]
    places = []
    for m in range(2):
        a = jnp.int32(0)
        for x in range(chips):
            a = jnp.where(chip == x, spots[m][x], a)
        mine = (a >= core * slots) & (a < (core + 1) * slots)
        places.append(jnp.where(mine, a - core * slots, slots + a - (1 - core) * slots))
    return goals, origin, near, ringed, left_over, places


def moe_kernel(group, map_ref, slot_ref, expert_ref, route_ref, gate_ref, tok_ref, wg_ref, wu_ref, wd_ref, sg_ref, su_ref, sd_ref,
               base_ref, first_ref, second_ref, pg_ref, pu_ref, pd_ref, arr_ref, far_ref,
               blk, part, rdir, rmrg, xin, wgb, wub, wdb, act, rbuf, gbuf, cbuf, cgot, ct, colb, pick, land, stage, inject_ref,
               ag_send, le_recv, la_recv, fw_send, fw_recv, co_send, co_recv, pw_send, pw_recv,
               di_send, di_recv, xi_send, xi_recv, mg_send, mg_recv, wg_sem, wu_sem, wd_sem, io_sem, out_sem, sum_sem,
               pick_sem, mv_send, mv_recv, arr_sem, far_send, far_recv):
    me = lax.axis_index('ep')
    core = lax.rem(me, CORES)
    chip = me // CORES
    right = lax.rem(me + CORES, group)
    left = lax.rem(me + group - CORES, group)
    across = lax.rem(me + 2 * CORES, group)
    mate = me + 1 - 2 * core
    rows_all, width = tok_ref.shape
    ffn = sg_ref.shape[2]
    layers = wg_ref.shape[0]
    slots = wg_ref.shape[1]
    piece = rows_all // CHUNKS
    half_rows = rows_all // 2
    total = layers * STEPS
    chips = group // CORES
    n_slots = group * slots

    def remote(src, dst, send, recv, dev):
        return pltpu.make_async_remote_copy(src_ref=src, dst_ref=dst, send_sem=send, recv_sem=recv,
                                            device_id={'ep': dev}, device_id_type=MESH)

    def rows(c):
        return pl.ds(pl.multiple_of(c * piece, piece), piece)

    def sums(c):
        size = half_rows // PIECES
        return pl.ds(pl.multiple_of(c * size, size), size)

    def halves(c, side):
        return sums(c + side * PIECES)

    def whole_half(side):
        return pl.ds(side * half_rows, half_rows)

    def lead_copy(side, c):
        at = rows(c + side * HALF)
        return remote(blk.at[0, at], blk.at[1, at], ag_send.at[side], le_recv.at[side, c], right if side == 0 else left)

    def late_copy(side, c):
        at = rows(c + (1 - side) * HALF)
        return remote(blk.at[0, at], blk.at[2, at], ag_send.at[side], la_recv.at[side], right if side == 0 else left)

    def forward_copy(side, c):
        at = rows(c + side * HALF)
        return remote(blk.at[1, at], blk.at[3, at], fw_send.at[side], fw_recv.at[side], right if side == 0 else left)

    def coef_copy(n):
        ahead, dev = ((1, right), (chips - 1, left), (2, across))[n]
        return remote(cbuf.at[lax.rem(chip + ahead, chips)], cgot.at[n], co_send, co_recv, dev)

    def direct_copy(side, c):
        return remote(part.at[1, halves(c, side)], rdir.at[side, sums(c)], di_send.at[side], di_recv.at[side],
                      left if side == 0 else right)

    def relay_copy(side, c):
        return remote(part.at[3, halves(c, side)], xin.at[side, sums(c)], xi_send.at[side],
                      xi_recv.at[side, jnp.maximum(c - EARLY, 0)], right if side == 0 else left)

    def merged_copy(side, c):
        return remote(part.at[2, halves(c, side)], rmrg.at[side, sums(c)], mg_send.at[side],
                      mg_recv.at[side, c // (PIECES // HALF)], right if side == 0 else left)

    def sum_out(side, c):
        return pltpu.make_async_copy(part.at[2, halves(c, side)], (first_ref, second_ref)[side].at[sums(c)], sum_sem.at[side])

    def base_out(side, c):
        d = halves(c, side)
        return pltpu.make_async_copy(part.at[0, d], base_ref.at[d], out_sem.at[side])

    def await_bytes(like, sem):
        pltpu.make_async_copy(like, like, sem).wait()

    def mate_copies(l, j):
        return [remote(src.at[l, j], dst.at[l, j], pw_send.at[n], pw_recv.at[l, j, n], mate)
                for n, (src, dst) in enumerate(((wg_ref, pg_ref), (wu_ref, pu_ref), (wd_ref, pd_ref)))]

    def step_kind(i):
        late = i - 5
        turn = late // 4
        unit = jnp.where(i < 5, 0, jnp.where(turn == 0, 1, 4 - turn))
        pos = jnp.where(i < 5, jnp.where(i < 2, i, jnp.where(i == 2, 4, i - 1)), late - 4 * turn)
        kind = jnp.where(pos == 4, 2, jnp.where(pos < 2, 0, 1))
        return unit, kind, jnp.where(pos == 4, 0, lax.rem(pos, 2))

    def fetch(n, which):
        l = n // STEPS
        i = n - l * STEPS
        _, kind, slot = step_kind(i)
        buf = lax.rem(n, 2)

        def go(g, u, d):
            if which == 0:
                pltpu.make_async_copy(g, wgb.at[buf], wg_sem.at[buf]).start()
                pltpu.make_async_copy(u, wub.at[buf], wu_sem.at[buf]).start()
            else:
                pltpu.make_async_copy(d, wdb, wd_sem).start()

        @pl.when(kind == 0)
        def _():
            go(wg_ref.at[l, slot], wu_ref.at[l, slot], wd_ref.at[l, slot])

        @pl.when(kind == 1)
        def _():
            go(pg_ref.at[l, slot], pu_ref.at[l, slot], pd_ref.at[l, slot])

        @pl.when(kind == 2)
        def _():
            go(sg_ref.at[l], su_ref.at[l], sd_ref.at[l])

    def columns(u, first, second):
        mine = jnp.concatenate([first[:, :half_rows], second[:, half_rows:]], axis=1)
        full = jnp.concatenate([mine, jnp.zeros((LANES - mine.shape[0], rows_all), F32)], axis=0)
        ct[u] = full.T

    def picks(l, t, side):
        tile = t if side == 0 else TILES - 1 - t
        at = lax.rem(tile, PER)
        across_ffn, across_half = ffn // TILE, PER // (ffn // TILE)

        def pair(own, other, r, c):
            spot = (pl.ds(pl.multiple_of(r, TILE), TILE), pl.ds(pl.multiple_of(c, TILE), TILE))
            return (pltpu.make_async_copy(own.at[(l, slice(None)) + spot], pick.at[side, pl.ds(0, slots)], pick_sem.at[side, 0]),
                    pltpu.make_async_copy(other.at[(l, slice(None)) + spot], pick.at[side, pl.ds(slots, slots)], pick_sem.at[side, 1]))

        mine = across_half * TILE * core
        tall = (mine + TILE * (at // across_ffn), TILE * lax.rem(at, across_ffn))
        wide = (TILE * (at // across_half), mine + TILE * lax.rem(at, across_half))
        up = pair(wu_ref, pu_ref, *tall)
        if side == 0:
            return (tile < PER, pair(wg_ref, pg_ref, *tall)), (tile >= PER, up)
        return (tile >= 2 * PER, pair(wd_ref, pd_ref, *wide)), (tile < 2 * PER, up)

    def pick_start(l, t):
        for side in range(2):
            for there, pair in picks(l, t, side):
                @pl.when(there)
                def _():
                    for copy in pair:
                        copy.start()

    def tile_copy(tick, side):
        return remote(stage.at[lax.rem(tick, 2), side], land.at[side, lax.rem(tick, RING)], mv_send.at[lax.rem(tick, 2), side],
                      mv_recv.at[side, lax.rem(tick, RING)], right if side == 0 else left)

    def tile_out(l, tick, side, begin):
        tile = land.at[side, lax.rem(tick, RING)]
        turn = lax.rem(tick, 2)
        keep = pltpu.make_async_copy(tile, arr_ref.at[l, side, tick], arr_sem.at[side, turn])
        give = remote(tile, far_ref.at[l, side, tick], far_send.at[side, turn], far_recv.at[l], mate)
        if begin:
            keep.start()
            give.start()
        else:
            keep.wait()
            give.wait_send()

    def ring_step(l, tick):
        inject = inject_ref[l]
        from_here = inject >= 0
        place = jnp.maximum(inject, 0)
        for side in range(2):
            for copy in picks(l, tick, side)[0][1]:
                copy.wait()

        for side in range(2):
            @pl.when(tick >= 2)
            def _():
                tile_copy(tick - 2, side).wait_send()

            @pl.when(tick >= 1)
            def _():
                tile_copy(tick - 1, side).wait_recv()
                tile_out(l, tick - 1, side, True)
                stage[lax.rem(tick, 2), side] = jnp.where(from_here, pick[side, place], land[side, lax.rem(tick + RING - 1, RING)])

            @pl.when(tick < 1)
            def _():
                stage[lax.rem(tick, 2), side] = pick[side, place]

        @pl.when(tick + 1 < TICKS)
        def _():
            pick_start(l, tick + 1)

        for side in range(2):
            @pl.when(tick > 1)
            def _():
                tile_out(l, tick - 2, side, False)

            tile_copy(tick, side).start()

    def beat(l, k):
        @pl.when(k < TICKS)
        def _():
            ring_step(l, k)

        @pl.when(k < HALF)
        def _():
            late_copy(0, k).start()
            late_copy(1, k).start()

        @pl.when((k >= HALF) & (k < HALF + PIECES))
        def _():
            direct_copy(0, k - HALF).start()
            direct_copy(1, k - HALF).start()

        @pl.when(k >= HALF + PIECES)
        def _():
            relay_copy(0, k - HALF - PIECES).start()
            relay_copy(1, k - HALF - PIECES).start()

    def ring_end(l):
        for side in range(2):
            tile_copy(jnp.int32(TICKS - 1), side).wait_recv()
            tile_out(l, jnp.int32(TICKS - 1), side, True)

    def ring_close(l):
        for side in range(2):
            for tick in range(TICKS - 2, TICKS):
                tile_out(l, jnp.int32(tick), side, False)
                tile_copy(jnp.int32(tick), side).wait_send()

    tok_in = pltpu.make_async_copy(tok_ref, blk.at[0], io_sem.at[0])
    route_in = pltpu.make_async_copy(route_ref, rbuf, io_sem.at[1])
    gate_in = pltpu.make_async_copy(gate_ref, gbuf, io_sem.at[2])
    tok_in.start()
    route_in.start()
    gate_in.start()
    fetch(jnp.int32(0), 0)
    fetch(jnp.int32(0), 1)

    barrier = pltpu.get_barrier_semaphore()
    for dev in (left, right, across, mate):
        pl.semaphore_signal(barrier, inc=1, device_id={'ep': dev}, device_id_type=MESH)
    pl.semaphore_wait(barrier, 4)

    tok_in.wait()
    for c in range(HALF):
        for side in range(2):
            lead_copy(side, c).start()
    for l in range(layers):
        for j in range(slots):
            for copy in mate_copies(l, j):
                copy.start()

    route_in.wait()
    gate_in.wait()
    for l in range(layers):
        for q in range(n_slots):
            expert = map_ref[l, q]
            serves = jnp.float32(1.0)
            for p in range(q):
                serves = jnp.where(map_ref[l, p] == expert, 0.0, serves)
            gates = jnp.sum(jnp.where(rbuf[l] == expert, gbuf[l], 0.0), axis=0, keepdims=True)
            at = slots * CORES * l + q % (slots * CORES)
            cbuf[q // (slots * CORES), at:at + 1, :] = gates * serves
    for n in range(3):
        coef_copy(n).start()
    columns(0, cbuf[chip], cbuf[chip])
    for l in range(layers):
        _, origin, _, ringed, _, places = read_plan(map_ref, slot_ref, expert_ref, l, chips, CORES * slots, chip, core, slots)
        sends = [ringed[m] & (origin[m] == chip) for m in range(2)]
        inject_ref[l] = jnp.where(sends[0], places[0], jnp.where(sends[1], places[1], -1))

    @pl.loop(0, layers)
    def layer(l):
        @pl.loop(0, STEPS)
        def step(i):
            n = l * STEPS + i
            unit, kind, slot = step_kind(i)
            buf = lax.rem(n, 2)

            for j, at in ((0, 2), (1, 3)):
                @pl.when(i == at)
                def _():
                    for copy in mate_copies(l, j):
                        copy.wait_recv()

            for at, pieces in ((2, (0,)), (3, (1, 2)), (4, (3,))):
                @pl.when(i == at)
                def _():
                    for c in pieces:
                        for side in range(2):
                            lead_copy(side, c).wait_recv()
                            forward_copy(side, c).start()

            @pl.when(i == 4)
            def _():
                pick_start(l, jnp.int32(0))

                @pl.when(l == 0)
                def _():
                    await_bytes(cgot, co_recv)
                    columns(1, cgot[0], cgot[1])
                    columns(2, cgot[1], cgot[0])
                    columns(3, cgot[2], cgot[2])

            @pl.when(i == 9)
            def _():
                for side in range(2):
                    await_bytes(blk.at[3, whole_half(side)], fw_recv.at[side])
                    await_bytes(blk.at[1, whole_half(side)], fw_send.at[side])

            @pl.when(i == 13)
            def _():
                for side in range(2):
                    await_bytes(blk.at[2, whole_half(1 - side)], la_recv.at[side])

            tick = jnp.where(i < FIRST + HALF, i - FIRST, HALF + 2 * (i - FIRST - HALF))

            @pl.when(i >= FIRST)
            def _():
                beat(l, tick)

            pltpu.make_async_copy(wg_ref.at[0, 0], wgb.at[buf], wg_sem.at[buf]).wait()
            pltpu.make_async_copy(wu_ref.at[0, 0], wub.at[buf], wu_sem.at[buf]).wait()

            @pl.when(n + 1 < total)
            def _():
                fetch(n + 1, 0)

            place = 4 * l + jnp.where(kind == 0, 2 * core, 2 * (1 - core)) + slot
            lane = lax.broadcasted_iota(jnp.int32, (rows_all, LANES), 1)
            col = jnp.sum(jnp.where(lane == place, ct[unit], 0.0), axis=1, keepdims=True)
            col = jnp.where(kind == 2, 1.0, col)
            colb[...] = jnp.broadcast_to(col, (rows_all, LANES))

            @pl.when(i == 0)
            def _():
                part[0] = blk[0].astype(F32)

            @pl.when((i == 5) | (i == 9) | (i == 13))
            def _():
                part[unit] = jnp.zeros((rows_all, width), F32)

            @pl.loop(0, ffn // 256)
            def _(f):
                cols = pl.ds(pl.multiple_of(f * 256, 256), 256)
                gate = jnp.dot(blk[unit], wgb[buf, :, cols], preferred_element_type=F32)
                up = jnp.dot(blk[unit], wub[buf, :, cols], preferred_element_type=F32)
                act[:, cols] = (gate / (1.0 + jnp.exp(-gate)) * up).astype(BF16)

            @pl.when(i >= FIRST + HALF)
            def _():
                beat(l, tick + 1)

            pltpu.make_async_copy(wd_ref.at[0, 0], wdb, wd_sem).wait()

            @pl.loop(0, width // 512)
            def _(w):
                cols = pl.ds(pl.multiple_of(w * 512, 512), 512)
                down = jnp.dot(act[...], wdb[:, cols], preferred_element_type=F32)
                scale = jnp.concatenate([colb[...]] * 4, axis=1)
                part[unit, :, cols] = part[unit, :, cols] + scale * down

            @pl.when(n + 1 < total)
            def _():
                fetch(n + 1, 1)

        for side in range(2):
            await_bytes(blk.at[0], ag_send.at[side])

        ring_end(l)

        def merge(c):
            for side in range(2):
                at = halves(c, side)
                part[2, at] = part[2, at] + xin[side, sums(c)]
            for side in range(2):
                @pl.when(l + 1 < layers)
                def _():
                    merged_copy(side, c).start()

                @pl.when(l + 1 == layers)
                def _():
                    sum_out(side, c).start()

        for side in range(2):
            await_bytes(xin.at[side, pl.ds(0, (EARLY + 1) * (half_rows // PIECES))], xi_recv.at[side, 0])

        pl.loop(0, EARLY + 1)(merge)

        @pl.loop(EARLY + 1, PIECES)
        def _(c):
            for side in range(2):
                relay_copy(side, c).wait_recv()
            merge(c)

        for side in range(2):
            await_bytes(rdir.at[side], di_recv.at[side])

        @pl.when(l + 1 < layers)
        def _():
            @pl.loop(0, HALF)
            def finish(c):
                for side in range(2):
                    await_bytes(rmrg.at[side, rows(c)], mg_recv.at[side, c])
                    d = rows(c + side * HALF)
                    blk[0, d] = (part[0, d] + rdir[side, rows(c)] + rmrg[side, rows(c)]).astype(BF16)
                for side in range(2):
                    lead_copy(side, c).start()

            for side in range(2):
                await_bytes(part.at[2, whole_half(side)], mg_send.at[side])

        @pl.when(l + 1 == layers)
        def _():
            @pl.loop(0, PIECES)
            def finish(c):
                for side in range(2):
                    d = halves(c, side)
                    part[0, d] = part[0, d] + rdir[side, sums(c)]
                for side in range(2):
                    base_out(side, c).start()

        ring_close(l)
        for side in range(2):
            await_bytes(part.at[1, whole_half(side)], di_send.at[side])
            await_bytes(part.at[3, whole_half(side)], xi_send.at[side])

    for side in range(2):
        await_bytes(part.at[2, whole_half(side)], sum_sem.at[side])
        await_bytes(part.at[0, whole_half(side)], out_sem.at[side])
    await_bytes(cgot, co_send)
    for l in range(layers):
        await_bytes(far_ref.at[l], far_recv.at[l])
    for n, ref in enumerate((pg_ref, pu_ref, pd_ref)):
        await_bytes(ref, pw_send.at[n])


def run_moe(group, old_map, move_slot, move_expert, routes, gates, tok, w_gate, w_up, w_down, sh_gate, sh_up, sh_down):
    n_rows, width = tok.shape
    layers, slots, _, ffn = w_gate.shape
    half = n_rows // 2
    chips = group // CORES
    any_spec = pl.BlockSpec(memory_space=pl.ANY)
    dma = pltpu.SemaphoreType.DMA
    flops = 2 * n_rows * 3 * width * ffn * layers * STEPS
    arrivals = jax.ShapeDtypeStruct((layers, 2, TICKS, TILE, TILE), BF16)
    return pl.pallas_call(
        functools.partial(moe_kernel, group),
        name='moe',
        out_shape=(jax.ShapeDtypeStruct(tok.shape, F32),) + (jax.ShapeDtypeStruct((half, width), F32),) * 2 + tuple(
            jax.ShapeDtypeStruct(w.shape, BF16) for w in (w_gate, w_up, w_down)) + (arrivals, arrivals),
        in_specs=[pl.BlockSpec(memory_space=pltpu.SMEM)] * 3 + [any_spec] * 9,
        out_specs=[any_spec] * 8,
        scratch_shapes=[
            pltpu.VMEM((chips, n_rows, width), BF16),
            pltpu.VMEM((chips, n_rows, width), F32),
            pltpu.VMEM((2, half, width), F32),
            pltpu.VMEM((2, half, width), F32),
            pltpu.VMEM((2, half, width), F32),
            pltpu.VMEM((2, width, ffn), BF16),
            pltpu.VMEM((2, width, ffn), BF16),
            pltpu.VMEM((ffn, width), BF16),
            pltpu.VMEM((n_rows, ffn), BF16),
            pltpu.VMEM(routes.shape, jnp.int32),
            pltpu.VMEM(gates.shape, F32),
            pltpu.VMEM((chips, layers * slots * CORES, n_rows), F32),
            pltpu.VMEM((chips - 1, layers * slots * CORES, n_rows), F32),
            pltpu.VMEM((chips, n_rows, LANES), F32),
            pltpu.VMEM((n_rows, LANES), F32),
            pltpu.VMEM((2, CORES * slots, TILE, TILE), BF16),
            pltpu.VMEM((2, RING, TILE, TILE), BF16),
            pltpu.VMEM((2, 2, TILE, TILE), BF16),
            pltpu.SMEM((layers,), jnp.int32),
            dma((2,)), dma((2, HALF)), dma((2,)), dma((2,)), dma((2,)), dma, dma,
            dma((3,)), dma((layers, slots, 3)),
            dma((2,)), dma((2,)), dma((2,)), dma((2, PIECES - EARLY)), dma((2,)), dma((2, HALF)),
            dma((2,)), dma((2,)), dma, dma((3,)), dma((2,)), dma((2,)),
            dma((2, 2)), dma((2, 2)), dma((2, RING)), dma((2, 2)), dma((2, 2)), dma((layers,)),
        ],
        compiler_params=pltpu.CompilerParams(collective_id=0, has_side_effects=True, vmem_limit_bytes=67043328),
        cost_estimate=pl.CostEstimate(flops=flops, bytes_accessed=400 * 2 ** 20, transcendentals=0),
    )(old_map, move_slot, move_expert, routes, gates, tok, w_gate, w_up, w_down, sh_gate, sh_up, sh_down)


KEEP, NEAR, RINGED = 0, 1, 2
DEPTH = 4


def place_kernel(group, map_ref, slot_ref, expert_ref, wg_ref, wu_ref, wd_ref, pg_ref, pu_ref, pd_ref, arr_ref, far_ref,
                 ng_ref, nu_ref, nd_ref, over_ref, tall, wide, in_sem, out_sem):
    layers, slots = wg_ref.shape[:2]
    me = lax.axis_index('ep')
    core = lax.rem(me, CORES)
    chip = me // CORES
    chips = group // CORES
    table = {}
    for l in range(layers):
        goals, origin, near, ringed, left_over, places = read_plan(map_ref, slot_ref, expert_ref, l, chips, CORES * slots, chip, core, slots)
        over_ref[l] = left_over.astype(jnp.int32)
        for j in range(slots):
            mode, pos, first, second = KEEP, 0, 0, 0
            for m in range(2):
                here = slot_ref[l, m] == me * slots + j
                ahead = lax.rem(goals[m] - origin[m] + chips, chips)
                mode = jnp.where(here, jnp.where(near[m], NEAR, jnp.where(ringed[m], RINGED, KEEP)), mode)
                pos = jnp.where(here, places[m], pos)
                first = jnp.where(here, ahead - 1, first)
                second = jnp.where(here, chips - ahead - 1, second)
            table[l, j] = mode, pos, (first, second)
    jobs = [(l, j, n) for l in range(layers) for j in range(slots) for n in range(3)]

    def parts(k):
        l, j, n = jobs[k]
        own = (wg_ref, wu_ref, wd_ref)[n]
        other = (pg_ref, pu_ref, pd_ref)[n]
        new = (ng_ref, nu_ref, nd_ref)[n]
        buf = (wide if n == 2 else tall).at[k % DEPTH]
        return l, j, n, own, other, new, buf

    def load(k):
        l, j, n, own, other, new, buf = parts(k)
        mode, pos, starts = table[l, j]
        sem = in_sem.at[k % DEPTH]

        @pl.when(mode == KEEP)
        def _():
            pltpu.make_async_copy(own.at[l, j], buf, sem).start()

        @pl.when((mode == NEAR) & (pos < slots))
        def _():
            pltpu.make_async_copy(own.at[l, pos], buf, sem).start()

        @pl.when((mode == NEAR) & (pos >= slots))
        def _():
            pltpu.make_async_copy(other.at[l, pos - slots], buf, sem).start()

        @pl.when(mode == RINGED)
        def _():
            across_ffn, across_half = wg_ref.shape[3] // TILE, PER // (wg_ref.shape[3] // TILE)
            for source, owner in ((arr_ref, core), (far_ref, 1 - core)):
                mine = across_half * TILE * owner

                @pl.loop(0, PER)
                def _(t):
                    tile = PER * n + t
                    one = tile < TICKS - starts[0]
                    side = jnp.where(one, 0, 1)
                    tick = jnp.where(one, tile + starts[0], TILES - 1 - tile + starts[1])
                    if n == 2:
                        r, c = TILE * (t // across_half), mine + TILE * lax.rem(t, across_half)
                    else:
                        r, c = mine + TILE * (t // across_ffn), TILE * lax.rem(t, across_ffn)
                    spot = (pl.ds(pl.multiple_of(r, TILE), TILE), pl.ds(pl.multiple_of(c, TILE), TILE))
                    pltpu.make_async_copy(source.at[l, side, tick], buf.at[spot], sem).start()

    def arrive(k):
        l, j, n, own, other, new, buf = parts(k)
        pltpu.make_async_copy(own.at[l, j], buf, in_sem.at[k % DEPTH]).wait()

    def store(k):
        l, j, n, own, other, new, buf = parts(k)
        return pltpu.make_async_copy(buf, new.at[l, j], out_sem.at[k % DEPTH])

    ahead = DEPTH - 1
    for k in range(ahead):
        load(k)
    for k in range(len(jobs)):
        arrive(k)
        store(k).start()
        if k >= 1:
            store(k - 1).wait()
        if k + ahead < len(jobs):
            load(k + ahead)
    store(len(jobs) - 1).wait()


def run_place(group, old_map, move_slot, move_expert, w_gate, w_up, w_down, p_gate, p_up, p_down, arrived, far):
    layers, _, width, ffn = w_gate.shape
    any_spec = pl.BlockSpec(memory_space=pl.ANY)
    smem = pl.BlockSpec(memory_space=pltpu.SMEM)
    dma = pltpu.SemaphoreType.DMA
    return pl.pallas_call(
        functools.partial(place_kernel, group),
        name='place',
        out_shape=tuple(jax.ShapeDtypeStruct(w.shape, BF16) for w in (w_gate, w_up, w_down)) + (
            jax.ShapeDtypeStruct((layers,), jnp.int32),),
        in_specs=[smem] * 3 + [any_spec] * 8,
        out_specs=[any_spec] * 3 + [smem],
        scratch_shapes=[pltpu.VMEM((DEPTH, width, ffn), BF16), pltpu.VMEM((DEPTH, ffn, width), BF16), dma((DEPTH,)), dma((DEPTH,))],
        compiler_params=pltpu.CompilerParams(vmem_limit_bytes=48 * 2 ** 20),
        cost_estimate=pl.CostEstimate(flops=2 * 10 ** 10, bytes_accessed=80 * 10 ** 6, transcendentals=0),
    )(old_map, move_slot, move_expert, w_gate, w_up, w_down, p_gate, p_up, p_down, arrived, far)


def finish_moves(group, news, weights, over, old_map, move_slot, move_expert):
    layers, n_slots = old_map.shape
    slots = weights[0].shape[1]
    ring = [(d, (d + 1) % group) for d in range(group)]

    def one(k, news):
        me = lax.axis_index('ep')
        l = jnp.where(over[0] > 0, k, layers - 1)
        ids = jnp.arange(n_slots, dtype=jnp.int32)
        source = jnp.min(jnp.where(old_map[l] == move_expert[l, 1], ids, n_slots))
        here = source // slots == me
        there = move_slot[l, 1] // slots == me
        index = move_slot[l, 1] % slots
        own = tuple(w[l, source % slots] for w in weights)

        def hop(_, held):
            return tuple(jnp.where(here, o, lax.ppermute(h, 'ep', ring)) for o, h in zip(own, held))

        got = lax.fori_loop(0, group - 1, hop, own)
        return tuple(new.at[l, index].set(jnp.where(there, g, new[l, index])) for new, g in zip(news, got))

    return lax.fori_loop(0, jnp.sum(over), one, news)


def solution(mesh):
    group = mesh.shape['ep']

    def body(tok_in, routes, gate_vals, w_gate, w_up, w_down, sh_gate, sh_up, sh_down, old_map, move_slot, move_expert):
        maps = (old_map, move_slot, move_expert)
        by_choice = (routes.transpose(0, 2, 1), gate_vals.transpose(0, 2, 1))
        base, first, second, p_gate, p_up, p_down, arrived, far = run_moe(group, *maps, *by_choice, tok_in, w_gate, w_up, w_down, sh_gate, sh_up, sh_down)
        *news, over = run_place(group, *maps, w_gate, w_up, w_down, p_gate, p_up, p_down, arrived, far)
        news = finish_moves(group, tuple(news), (w_gate, w_up, w_down), over, *maps)
        rightward = [(d, (d + CORES) % group) for d in range(group)]
        leftward = [(d, (d + group - CORES) % group) for d in range(group)]
        hidden = (base + jnp.concatenate([lax.ppermute(first, 'ep', rightward), lax.ppermute(second, 'ep', leftward)], axis=0)).astype(BF16)
        return (hidden,) + tuple(news)

    weight_spec = P(None, TOKEN_AXES, None, None)
    route_spec = P(None, TOKEN_AXES, None)
    map_spec = P(None, 'replica')
    shared_spec = P(None, None, None)
    tok_spec = P(TOKEN_AXES, None)
    return jax.shard_map(body, mesh=mesh, in_specs=(tok_spec, route_spec, route_spec, weight_spec, weight_spec, weight_spec, shared_spec, shared_spec, shared_spec, map_spec, map_spec, map_spec), out_specs=(tok_spec, weight_spec, weight_spec, weight_spec), check_vma=False)
```
